128 devices in a mesh: dp: 16 (over x_lo, y, core), mp: 8 (over x_hi, z).
Axes of the slice: x: 4 (x_hi: 2, x_lo: 2; x = x_hi * 2 + x_lo), y: 4, z: 4, core: 2. Of those that a mesh axis runs over, the one named last changes fastest.
Arguments:
- tokens: bfloat16 [4096, 6144], P('dp', 'mp'), may hold values from -40 to 40
- norm_gain: float32 [6144], P('mp'), may hold values from 0.1 to 1.9
- w_qkv: bfloat16 [6144, 3, 4096], P('mp', None, 'dp'), may hold values from -0.078125 to 0.078125
- w_up: bfloat16 [6144, 12288], P('mp', 'dp'), may hold values from -0.078125 to 0.078125
- w_attn_out: bfloat16 [4096, 6144], P('dp', 'mp'), may hold values from -0.09375 to 0.09375
- w_down: bfloat16 [12288, 6144], P('dp', 'mp'), may hold values from -0.0546875 to 0.0546875
Outputs:
- layer_out: bfloat16 [4096, 6144], P('dp', 'mp')
The draws below stay inside these ranges and needn't reach their ends.
All inputs are finite; a program needn't handle non-finite values.
Results may differ from the reference program's by a relative error of at most 0.015.
Values may be sent and summed in bfloat16 or wider, within the bound.
A program may use at most 128 MiB of HBM per device.

```python
import jax
import jax.numpy as jnp
from jax import lax

D = 6144
HEADS = 32
HEAD_DIM = 128
FF = 12288
PATCHES = 256
TOKENS = 4096
N_DP = 16
N_MP = 8


def draw_tokens(key, part):
    first = jax.random.fold_in(key, 0)
    ramp = 0.6 * 3.0 ** (jnp.arange(D, dtype=jnp.float32) / D)
    values = jnp.clip(jax.random.normal(first, (TOKENS, D), jnp.float32), -6.0, 6.0) * ramp[None, :]
    return values.astype(jnp.bfloat16)


def levels(own_key, extent, pieces, low, largest):
    level = 1.0
    for dim, blocks in pieces:
        steps = jax.random.uniform(jax.random.fold_in(jax.random.fold_in(own_key, 6), dim), (blocks,), jnp.float32, low / len(pieces), largest / len(pieces))
        level = level * jnp.repeat(jnp.exp(steps), extent[dim] // blocks).reshape((-1,) + (1,) * (len(extent) - 1 - dim))
    return level


def bell_draw(rng, dims, deviation, most, pieces=(), held_as=jnp.bfloat16):
    loudness = levels(rng, dims, pieces, -0.22, 0.18) if pieces else 1.0
    drawn = jax.random.normal(rng, dims, jnp.float32) * deviation * loudness
    return jnp.minimum(jnp.maximum(drawn, -most), most).astype(held_as)


def setup_inputs(seed: int = 0) -> dict:
    splits = jax.random.split(jax.random.key(seed), 7)
    return {
        "tokens": draw_tokens(jax.random.fold_in(splits[6], 71), 0),
        "norm_gain": jnp.clip(1.0 + 0.18 * jax.random.normal(splits[1], (D,), jnp.float32), 0.1, 1.9),
        "w_qkv": bell_draw(splits[2], (D, 3, HEADS * HEAD_DIM), D ** -0.5, 0.078125, ((0, 8), (2, 16))),
        "w_up": bell_draw(splits[3], (D, FF), D ** -0.5, 0.078125, ((0, 8), (1, 16))),
        "w_attn_out": bell_draw(splits[4], (HEADS * HEAD_DIM, D), (HEADS * HEAD_DIM) ** -0.5, 0.09375, ((0, 16), (1, 8))),
        "w_down": bell_draw(splits[5], (FF, D), FF ** -0.5, 0.0546875, ((0, 16), (1, 8))),
    }


EPS = 1e-06

def normalize_rows(values, total, squares, gain, width):
    mean = total / width
    spread = squares / width - mean * mean
    scaled = (values - mean[:, None]) * lax.rsqrt(spread + EPS)[:, None]
    return (scaled * gain[None, :]).astype(jnp.bfloat16)

def head_norm(values):
    mean = lax.optimization_barrier(jnp.mean(values, axis=-1, keepdims=True))
    centered = values - mean
    spread = lax.optimization_barrier(jnp.mean(centered * centered, axis=-1, keepdims=True))
    return centered * lax.rsqrt(spread + EPS)

def attend(qkv, heads_here):
    rows = qkv.shape[0]
    images = rows // PATCHES
    parts = qkv.reshape(images, PATCHES, 3, heads_here, HEAD_DIM)
    query = (head_norm(parts[:, :, 0].astype(jnp.float32)) * (1.0 / HEAD_DIM) ** 0.5).astype(jnp.bfloat16)
    keys = head_norm(parts[:, :, 1].astype(jnp.float32)).astype(jnp.bfloat16)
    values = parts[:, :, 2]
    scores = jnp.einsum('iqhd,ikhd->ihqk', query.astype(jnp.float32), keys.astype(jnp.float32))
    weights = jnp.exp(scores)
    probs = (weights / lax.optimization_barrier(jnp.sum(weights, axis=-1, keepdims=True))).astype(jnp.bfloat16)
    mixed = jnp.einsum('ihqk,ikhd->iqhd', probs.astype(jnp.float32), values.astype(jnp.float32))
    return mixed.astype(jnp.bfloat16).reshape(rows, heads_here * HEAD_DIM)

def reference(tokens, norm_gain, w_qkv, w_up, w_attn_out, w_down):
    xf = tokens.astype(jnp.float32)
    normed = normalize_rows(xf, lax.optimization_barrier(jnp.sum(xf, axis=1)), lax.optimization_barrier(jnp.sum(xf * xf, axis=1)), norm_gain, D)
    head_cols = HEADS * HEAD_DIM
    w_heads = w_qkv.reshape(D, 3 * head_cols)
    feat_block = D // N_MP
    projected = jnp.zeros((TOKENS, 3 * head_cols + FF), jnp.float32)
    for block in range(N_MP):
        first = block * feat_block
        cols = normed[:, first:first + feat_block]
        term = jnp.concatenate([jnp.dot(cols, w_heads[first:first + feat_block], preferred_element_type=jnp.float32), jnp.dot(cols, w_up[first:first + feat_block], preferred_element_type=jnp.float32)], axis=1)
        projected = projected + lax.optimization_barrier(term.astype(jnp.bfloat16)).astype(jnp.float32)
    projected = projected.astype(jnp.bfloat16)
    qkv = projected[:, :3 * head_cols].reshape(TOKENS, 3, head_cols)
    attended = attend(qkv, HEADS)
    activated = jax.nn.gelu(projected[:, 3 * head_cols:].astype(jnp.float32)).astype(jnp.bfloat16)
    head_block = head_cols // N_DP
    unit_block = FF // N_DP
    total = xf
    for block in range(N_DP):
        hfirst = block * head_block
        ufirst = block * unit_block
        term = jnp.dot(attended[:, hfirst:hfirst + head_block], w_attn_out[hfirst:hfirst + head_block], preferred_element_type=jnp.float32)
        term = term + jnp.dot(activated[:, ufirst:ufirst + unit_block], w_down[ufirst:ufirst + unit_block], preferred_element_type=jnp.float32)
        total = total + lax.optimization_barrier(term.astype(jnp.bfloat16)).astype(jnp.float32)
    return total.astype(jnp.bfloat16)
```

```python
import functools

import jax
import jax.numpy as jnp
from jax import lax
from jax.experimental import pallas as pl
from jax.experimental.pallas import tpu as pltpu
from jax.sharding import Mesh
from jax.sharding import PartitionSpec as P

HEAD_DIM = 128
PATCHES = 256
EPS = 1e-06
MESH = pl.DeviceIdType.MESH
F32 = jnp.float32
BF16 = jnp.bfloat16
DP = ("L", "Y", "C")
MP = ("H", "Z")

CHUNKS = 3
RELS = (2, 1, 3, 0)
N_SEND = 160
N_RECV = 160


def gelu(u):
    return 0.5 * u * (1.0 + jnp.tanh(0.7978845608028654 * (u + 0.044715 * (u * u * u))))


def head_norm(values):
    mean = jnp.mean(values, axis=-1, keepdims=True)
    centered = values - mean
    spread = jnp.mean(centered * centered, axis=-1, keepdims=True)
    return centered * lax.rsqrt(spread + EPS)


def kernel(
    width,
    tok, stats, gain, w1, w_attn, w_down,
    out,
    statbuf, normed, xbuf, w1buf, w2buf, pbuf, r1, r2, qkv, hbuf, obuf, osend, osib, ry1, ry2, xsend, xrecv,
    send_sem, recv_sem,
):
    L, Y, C, H, Z = (lax.axis_index(a) for a in ("L", "Y", "C", "H", "Z"))
    rows, feat = tok.shape
    half = rows // 2
    wide = pbuf.shape[-1]
    lo = {"L": 1 - L}
    cross = {"L": 1 - L, "H": 1 - H}
    up, down = {"Y": lax.rem(Y + 1, 4)}, {"Y": lax.rem(Y + 3, 4)}
    fwd, back = {"Z": lax.rem(Z + 1, 4)}, {"Z": lax.rem(Z + 3, 4)}
    sib = {"C": 1 - C}
    swapped = (C != H).astype(jnp.int32)

    count = {"s": 0, "r": 0}
    pending = []

    def sems(kind, n=1):
        first = count[kind]
        count[kind] += n
        return first

    def copy(src, dst, recv, dev):
        d = pltpu.make_async_remote_copy(
            src_ref=src, dst_ref=dst, send_sem=send_sem.at[sems("s")], recv_sem=recv_sem.at[recv],
            device_id=dev, device_id_type=MESH,
        )
        d.start()
        pending.append(d)

    def arrive(dst, recv):
        pltpu.make_async_remote_copy(
            src_ref=dst, dst_ref=dst, send_sem=send_sem.at[0], recv_sem=recv_sem.at[recv],
            device_id=sib, device_id_type=MESH,
        ).wait_recv()

    barrier = pltpu.get_barrier_semaphore()
    offsets = [(dh, dz) for dh in range(2) for dz in range(4) if dh + dz]
    peers = [{"H": lax.rem(H + dh, 2), "Z": lax.rem(Z + dz, 4)} for dh, dz in offsets]
    for dev in peers + [lo, cross, up, down, sib]:
        pl.semaphore_signal(barrier, inc=1, device_id=dev, device_id_type=MESH)

    @pl.when(C != H)
    def _():
        for b in range(2):
            pl.semaphore_signal(barrier, inc=1, device_id={"H": C, "L": b, "C": H}, device_id_type=MESH)

    pl.semaphore_wait(barrier, 12 + 2 * swapped)

    stat_r = sems("r", 7)
    for k, dev in enumerate(peers):
        copy(stats, statbuf.at[k], stat_r + k, dev)

    w1_r = sems("r", 2 * CHUNKS)

    def send_w1(j):
        copy(w1.at[j], w1buf.at[H, j], w1_r + j, lo)
        copy(w1.at[j], w1buf.at[H, j], w1_r + CHUNKS + j, cross)

    for k in range(7):
        arrive(statbuf.at[k], stat_r + k)
    summed = stats[...]
    for k in range(7):
        summed = summed + statbuf[k]
    column = jnp.transpose(jnp.concatenate([summed] * 16, axis=0))
    mean = column[:, 0:1] / width
    spread = column[:, 1:2] / width - mean * mean
    scale = lax.rsqrt(spread + EPS)
    normed[...] = ((tok[...].astype(F32) - mean) * scale * gain[...]).astype(BF16)

    x_r = sems("r", 2)
    x_s = sems("s", 2)

    def token_copy(b):
        return pltpu.make_async_remote_copy(
            src_ref=normed, dst_ref=xbuf.at[H, 0, L], send_sem=send_sem.at[x_s + b], recv_sem=recv_sem.at[x_r + L],
            device_id={"H": C, "L": b, "C": H}, device_id_type=MESH,
        )

    for b in range(2):
        mine = jnp.logical_and(C == H, L == b)

        @pl.when(mine)
        def _():
            xbuf[H, 0, b] = normed[...]

        @pl.when(jnp.logical_not(mine))
        def _():
            token_copy(b).start()

    for j in range(CHUNKS):
        send_w1(j)
    w2_r = sems("r", 8)
    for n, dev in enumerate((lo, cross)):
        for h in range(2):
            units = w_down.shape[0] // 2
            copy(w_attn.at[pl.ds(h * 128, 128)], w2buf.at[H, h, pl.ds(0, 128)], w2_r + 4 * n + 2 * h, dev)
            copy(w_down.at[pl.ds(h * units, units)], w2buf.at[H, h, pl.ds(128, units)], w2_r + 4 * n + 2 * h + 1, dev)

    yp_r, ym_r, ya_r, yb_r, sib_r = sems("r", 2), sems("r", 2), sems("r", 2), sems("r", 2), sems("r", 8)

    def to_sib(rel, b):
        copy(xbuf.at[C, rel, b], xbuf.at[C, rel, b], sib_r + 2 * rel + b, sib)

    for b in range(2):

        @pl.when(jnp.logical_not(jnp.logical_and(C == H, L == b)))
        def _():
            arrive(xbuf.at[C, 0, b], x_r + b)

        copy(xbuf.at[C, 0, b], xbuf.at[C, 3, b], yp_r + b, up)
        copy(xbuf.at[C, 0, b], xbuf.at[C, 1, b], ym_r + b, down)
        to_sib(0, b)
    for b in range(2):
        arrive(xbuf.at[C, 3, b], yp_r + b)
        copy(xbuf.at[C, 3, b, pl.ds(0, half)], xbuf.at[C, 2, b, pl.ds(0, half)], ya_r + b, up)
        to_sib(3, b)
        arrive(xbuf.at[C, 1, b], ym_r + b)
        copy(xbuf.at[C, 1, b, pl.ds(half, half)], xbuf.at[C, 2, b, pl.ds(half, half)], yb_r + b, down)
        to_sib(1, b)
    for b in range(2):
        arrive(xbuf.at[C, 2, b, pl.ds(0, half)], ya_r + b)
        arrive(xbuf.at[C, 2, b, pl.ds(half, half)], yb_r + b)
        to_sib(2, b)

    items = [(j, rel) for j in range(CHUNKS) for rel in RELS]
    n_items = len(items)
    r1a_r, r1b_r, r2p_r, r2m_r = (sems("r", n_items) for _ in range(4))
    dp_r, dm_r, da_r, db_r = (sems("r", 8) for _ in range(4))
    e_r = sems("r", 4)
    zp, zm, z2 = lax.rem(Z + 1, 4), lax.rem(Z + 3, 4), lax.rem(Z + 2, 4)
    seen_w, seen_x = set(), set()

    def s1(i):
        j, rel = items[i]
        if j not in seen_w:
            seen_w.add(j)
            arrive(w1buf.at[H, j], w1_r + j)
            arrive(w1buf.at[1 - H, j], w1_r + CHUNKS + j)
        if rel not in seen_x:
            seen_x.add(rel)
            for b in range(2):
                arrive(xbuf.at[1 - C, rel, b], sib_r + 2 * rel + b)

        @pl.loop(0, 4)
        def _(q):
            h, b = q // 2, q % 2
            acc = jnp.dot(xbuf[0, rel, b], w1buf[0, j, h], preferred_element_type=F32)
            acc = acc + jnp.dot(xbuf[1, rel, b], w1buf[1, j, h], preferred_element_type=F32)
            pbuf[i, q] = acc.astype(BF16)

        copy(pbuf.at[i, z2, pl.ds(0, half)], r1.at[0, i], r1a_r + i, fwd)
        copy(pbuf.at[i, z2, pl.ds(half, half)], r1.at[1, i], r1b_r + i, back)

    def s2(i):
        arrive(r1.at[0, i], r1a_r + i)
        pbuf[i, zp, pl.ds(0, half)] = (pbuf[i, zp, pl.ds(0, half)].astype(F32) + r1[0, i].astype(F32)).astype(BF16)
        copy(pbuf.at[i, zp], r2.at[0, i], r2p_r + i, fwd)
        arrive(r1.at[1, i], r1b_r + i)
        pbuf[i, zm, pl.ds(half, half)] = (
            pbuf[i, zm, pl.ds(half, half)].astype(F32) + r1[1, i].astype(F32)
        ).astype(BF16)
        copy(pbuf.at[i, zm], r2.at[1, i], r2m_r + i, back)

    def s3(i):
        j, rel = items[i]
        arrive(r2.at[0, i], r2p_r + i)
        arrive(r2.at[1, i], r2m_r + i)
        whole = (pbuf[i, Z].astype(F32) + r2[0, i].astype(F32) + r2[1, i].astype(F32)).astype(BF16)
        if j == 0:
            qkv[rel] = whole
            return
        if j == 1:
            both = qkv[rel].astype(F32)
            query = (head_norm(both[:, :HEAD_DIM]) * (1.0 / HEAD_DIM) ** 0.5).astype(BF16)
            keys = head_norm(both[:, HEAD_DIM:]).astype(BF16)
            scores = lax.dot_general(query, keys, (((1,), (1,)), ((), ())), preferred_element_type=F32)
            weights = jnp.exp(scores)
            probs = (weights / jnp.sum(weights, axis=-1, keepdims=True)).astype(BF16)
            mixed = jnp.dot(probs, whole[:, :HEAD_DIM], preferred_element_type=F32)
            hbuf[rel, Z, 0, :, pl.ds(0, HEAD_DIM)] = mixed.astype(BF16)
            hbuf[rel, Z, 0, :, pl.ds(HEAD_DIM, HEAD_DIM)] = gelu(whole[:, HEAD_DIM:].astype(F32)).astype(BF16)
        else:
            hbuf[rel, Z, 1] = gelu(whole.astype(F32)).astype(BF16)
        k = j - 1
        copy(hbuf.at[rel, Z, k], hbuf.at[rel, Z, k], dp_r + 2 * rel + k, fwd)
        copy(hbuf.at[rel, Z, k], hbuf.at[rel, Z, k], dm_r + 2 * rel + k, back)

    def relay(i):
        j, rel = items[i]
        if j == 0:
            return
        k = j - 1
        arrive(hbuf.at[rel, zm, k], dp_r + 2 * rel + k)
        top = hbuf.at[rel, zm, k, pl.ds(0, half)]
        copy(top, top, da_r + 2 * rel + k, fwd)
        arrive(hbuf.at[rel, zp, k], dm_r + 2 * rel + k)
        low = hbuf.at[rel, zp, k, pl.ds(half, half)]
        copy(low, low, db_r + 2 * rel + k, back)

    seen_w2 = []

    def e1(rel):
        if not seen_w2:
            seen_w2.append(1)
            units = w_down.shape[0] // 2
            for n, src in enumerate((H, 1 - H)):
                for h in range(2):
                    arrive(w2buf.at[src, h, pl.ds(0, 128)], w2_r + 4 * n + 2 * h)
                    arrive(w2buf.at[src, h, pl.ds(128, units)], w2_r + 4 * n + 2 * h + 1)
        for k in range(2):
            arrive(hbuf.at[rel, z2, k, pl.ds(0, half)], da_r + 2 * rel + k)
            arrive(hbuf.at[rel, z2, k, pl.ds(half, half)], db_r + 2 * rel + k)

        def product(f, b):
            acc = None
            for h in range(2):
                for k in range(2):
                    term = jnp.dot(
                        hbuf[rel, 2 * h + b, k], w2buf[f, h, pl.ds(k * 256, 256)], preferred_element_type=F32
                    )
                    acc = term if acc is None else acc + term
            return acc.astype(BF16)

        @pl.loop(0, 2)
        def _(b):
            osend[rel, b] = product(1 - C, b)

        copy(osend.at[rel], osib.at[rel], e_r + rel, sib)

        @pl.loop(0, 2)
        def _(b):
            obuf[rel, b] = product(C, b)

    ry_r = sems("r", 4)
    xr_r = sems("r", 2)
    xr_s = sems("s", 2)

    def final_copy(b):
        return pltpu.make_async_remote_copy(
            src_ref=xsend.at[b], dst_ref=xrecv.at[L], send_sem=send_sem.at[xr_s + b], recv_sem=recv_sem.at[xr_r + L],
            device_id={"H": C, "L": b, "C": H}, device_id_type=MESH,
        )

    def e2(rel):
        arrive(osib.at[rel], e_r + rel)
        for b in range(2):
            total = obuf[rel, b].astype(F32) + osib[rel, b].astype(F32)
            if rel == 1 and b == 0:
                arrive(ry1.at[0], ry_r)
                total = total + ry1[0].astype(F32)
            if rel == 3 and b == 1:
                arrive(ry1.at[1], ry_r + 1)
                total = total + ry1[1].astype(F32)
            if rel == 0:
                if b == 0:
                    arrive(ry2.at[0], ry_r + 2)
                    arrive(ry2.at[1], ry_r + 3)
                xsend[b] = (total + ry2[0, b].astype(F32) + ry2[1, b].astype(F32)).astype(BF16)
                mine = jnp.logical_and(C == H, L == b)

                @pl.when(mine)
                def _():
                    xrecv[b] = xsend[b]

                @pl.when(jnp.logical_not(mine))
                def _():
                    final_copy(b).start()
            else:
                obuf[rel, b] = total.astype(BF16)
        if rel == 2:
            copy(obuf.at[2, 0], ry1.at[0], ry_r, up)
            copy(obuf.at[2, 1], ry1.at[1], ry_r + 1, down)
        if rel == 1:
            copy(obuf.at[1], ry2.at[0], ry_r + 2, up)
        if rel == 3:
            copy(obuf.at[3], ry2.at[1], ry_r + 3, down)

    first_last = n_items - 4
    for t in range(n_items + 6):
        if t < n_items:
            s1(t)
        if 0 <= t - 1 < n_items:
            s2(t - 1)
        if 0 <= t - 2 < n_items:
            s3(t - 2)
        if 0 <= t - 3 < n_items:
            relay(t - 3)
        if first_last <= t - 4 < n_items:
            e1(items[t - 4][1])
        if first_last <= t - 5 < n_items:
            e2(items[t - 5][1])

    for b in range(2):

        @pl.when(jnp.logical_not(jnp.logical_and(C == H, L == b)))
        def _():
            arrive(xrecv.at[b], xr_r + b)

    out[...] = (tok[...].astype(F32) + xrecv[0].astype(F32) + xrecv[1].astype(F32)).astype(BF16)

    for d in pending:
        d.wait_send()
    for b in range(2):

        @pl.when(jnp.logical_not(jnp.logical_and(C == H, L == b)))
        def _():
            token_copy(b).wait_send()
            final_copy(b).wait_send()

    assert count["s"] <= N_SEND and count["r"] <= N_RECV, count


def local(tokens, norm_gain, w_qkv, w_up, w_attn_out, w_down):
    rows, feat = tokens.shape
    width = feat * lax.axis_size("H") * lax.axis_size("Z")
    tokens_f = tokens.astype(F32)
    sums = jnp.stack([jnp.sum(tokens_f, axis=1), jnp.sum(tokens_f * tokens_f, axis=1)])
    stats = jnp.concatenate([sums, jnp.zeros((6, rows), F32)], axis=0)
    units = w_up.shape[1] // 2
    by_head = jnp.concatenate(
        [
            w_qkv.reshape(feat, 3, 2, HEAD_DIM).transpose(2, 0, 1, 3).reshape(2, feat, 3 * HEAD_DIM),
            w_up.reshape(feat, 2, units).transpose(1, 0, 2),
        ],
        axis=2,
    )
    wide = by_head.shape[2] // CHUNKS
    w1 = by_head.reshape(2, feat, CHUNKS, wide).transpose(2, 0, 1, 3)
    n_items = 4 * CHUNKS
    half = rows // 2
    vmem = pltpu.VMEM
    scratch = [
        vmem((7, 8, rows), F32),
        vmem((rows, feat), BF16),
        vmem((2, 4, 2, rows, feat), BF16),
        vmem((2, CHUNKS, 2, feat, wide), BF16),
        vmem((2, 2, 512, feat), BF16),
        vmem((n_items, 4, rows, wide), BF16),
        vmem((2, n_items, half, wide), BF16),
        vmem((2, n_items, rows, wide), BF16),
        vmem((4, rows, wide), BF16),
        vmem((4, 4, 2, rows, 256), BF16),
        vmem((4, 2, rows, feat), BF16),
        vmem((4, 2, rows, feat), BF16),
        vmem((4, 2, rows, feat), BF16),
        vmem((2, rows, feat), BF16),
        vmem((2, 2, rows, feat), BF16),
        vmem((2, rows, feat), BF16),
        vmem((2, rows, feat), BF16),
        pltpu.SemaphoreType.DMA((N_SEND,)),
        pltpu.SemaphoreType.DMA((N_RECV,)),
    ]
    in_vmem = pl.BlockSpec(memory_space=pltpu.VMEM)
    anywhere = pl.BlockSpec(memory_space=pl.ANY)
    return pl.pallas_call(
        functools.partial(kernel, width),
        out_shape=jax.ShapeDtypeStruct((rows, feat), BF16),
        in_specs=[in_vmem] * 3 + [anywhere] * 3,
        out_specs=in_vmem,
        scratch_shapes=scratch,
        compiler_params=pltpu.CompilerParams(
            collective_id=0, has_side_effects=True, vmem_limit_bytes=60 * 1024 * 1024
        ),
        name="layer",
    )(tokens, stats, norm_gain[None, :], w1, w_attn_out, w_down)


def solution(mesh):
    torus = Mesh(mesh.devices.reshape(2, 4, 2, 2, 4), ("L", "Y", "C", "H", "Z"))
    in_specs = (P(DP, MP), P(MP), P(MP, None, DP), P(MP, DP), P(DP, MP), P(DP, MP))
    return jax.shard_map(local, mesh=torus, in_specs=in_specs, out_specs=P(DP, MP), check_vma=False)
```

```python
import functools

import jax
import jax.numpy as jnp
from jax import lax
from jax.experimental import pallas as pl
from jax.experimental.pallas import tpu as pltpu
from jax.sharding import Mesh
from jax.sharding import PartitionSpec as P

HEAD_DIM = 128
PATCHES = 256
EPS = 1e-06
MESH = pl.DeviceIdType.MESH
F32 = jnp.float32
BF16 = jnp.bfloat16
DP = ("L", "Y", "C")
MP = ("H", "Z")

CHUNKS = 6
WIDE = 2 * HEAD_DIM
PARTS = 3
ITEMS = (
    (0, 0), (1, 0), (0, 1), (0, 3), (1, 1), (1, 3), (2, 1), (2, 3), (0, 2), (1, 2), (2, 2), (3, 2), (3, 1), (4, 2),
    (5, 2), (4, 1), (5, 1), (3, 3), (4, 3), (5, 3), (2, 0), (3, 0), (4, 0), (5, 0),
)
LAGS = (2, 4, 6)
FAR_STEP = 8
OUT_STEPS = (
    (22, 1, 2, 0), (23, 2, 2, 0), (23, 1, 2, 1), (24, 2, 2, 1), (24, 1, 1, 0), (24, 1, 1, 1), (25, 2, 1, 0),
    (25, 1, 2, 2), (25, 1, 1, 2), (26, 2, 2, 2), (26, 2, 1, 1), (27, 1, 3, 0), (27, 1, 3, 1), (27, 1, 3, 2),
    (28, 2, 1, 2), (28, 2, 3, 0), (28, 2, 3, 1), (28, 2, 3, 2), (31, 1, 0, 0), (31, 1, 0, 1), (31, 2, 0, 0),
    (31, 1, 0, 2), (31, 2, 0, 1), (31, 2, 0, 2),
)
N_SEND = 224
N_RECV = 224


def gelu(u):
    return 0.5 * u * (1.0 + jnp.tanh(0.7978845608028654 * (u + 0.044715 * (u * u * u))))


def head_norm(values):
    mean = jnp.mean(values, axis=-1, keepdims=True)
    centered = values - mean
    spread = jnp.mean(centered * centered, axis=-1, keepdims=True)
    return centered * lax.rsqrt(spread + EPS)


def kernel(
    width,
    tok, gain, w_qkv, w_up, w_attn, w_down,
    out,
    stats, statbuf, xraw, xbuf, w1buf, w2buf, pbuf, r1, r2, qkv, hbuf, obuf, osend, osib, ry1, ry2, xsend, xrecv,
    send_sem, recv_sem,
):
    L, Y, C, H, Z = (lax.axis_index(a) for a in ("L", "Y", "C", "H", "Z"))
    rows, feat = tok.shape
    half = rows // 2
    near = ({"L": 1 - L, "H": C}, {"L": 1 - L, "H": 1 - C})
    up, down = {"Y": lax.rem(Y + 1, 4)}, {"Y": lax.rem(Y + 3, 4)}
    fwd, back = {"Z": lax.rem(Z + 1, 4)}, {"Z": lax.rem(Z + 3, 4)}
    sib = {"C": 1 - C}
    swapped = (C != H).astype(jnp.int32)
    straight = C == H

    count = {"s": 0, "r": 0}
    pending = []

    def sems(kind, n=1):
        first = count[kind]
        count[kind] += n
        return first

    def copy(src, dst, recv, dev):
        d = pltpu.make_async_remote_copy(
            src_ref=src, dst_ref=dst, send_sem=send_sem.at[sems("s")], recv_sem=recv_sem.at[recv],
            device_id=dev, device_id_type=MESH,
        )
        d.start()
        pending.append(d)

    def arrive(dst, recv):
        pltpu.make_async_remote_copy(
            src_ref=dst, dst_ref=dst, send_sem=send_sem.at[0], recv_sem=recv_sem.at[recv],
            device_id=sib, device_id_type=MESH,
        ).wait_recv()

    barrier = pltpu.get_barrier_semaphore()
    for dev in (*near, up, down, fwd, back, sib):
        pl.semaphore_signal(barrier, inc=1, device_id=dev, device_id_type=MESH)

    readers = [(dl, dz, dc) for dl in range(2) for dz in range(4) for dc in range(2)]

    def reader(dl, dz, dc):
        return {"H": C, "L": lax.rem(L + dl, 2), "Z": lax.rem(Z + dz, 4), "C": lax.rem(C + dc, 2)}

    def unless(condition, skip, f):
        if skip:
            pl.when(jnp.logical_not(condition))(f)
        else:
            f()

    for dh, dl, dz in [(dh, dl, dz) for dh in range(2) for dl in range(2) for dz in range(4)]:

        def greet():
            source = {"C": H, "H": lax.rem(H + dh, 2), "L": lax.rem(L + dl, 2), "Z": lax.rem(Z + dz, 4)}
            pl.semaphore_signal(barrier, inc=1, device_id=source, device_id_type=MESH)

        unless(straight, dh + dl + dz == 0, greet)

    w1_r = sems("r", 2 * CHUNKS)
    w2_r = sems("r", 2 * PARTS)

    def send_w1(j, dev):
        block = w_qkv.at[j] if j < 3 else w_up.at[:, pl.ds((j - 3) * WIDE, WIDE)]
        copy(block, w1buf.at[H, j], w1_r + H * CHUNKS + j, dev)

    def send_w2(f, dev):
        top, columns = w_attn.shape[0], pl.ds(f * WIDE, WIDE)
        copy(w_attn.at[:, columns], w2buf.at[H, f, pl.ds(0, top)], w2_r + H * PARTS + f, dev)
        copy(w_down.at[:, columns], w2buf.at[H, f, pl.ds(top, w_down.shape[0])], w2_r + H * PARTS + f, dev)

    tokens_f = tok[...].astype(F32)
    lane = lax.broadcasted_iota(jnp.int32, (rows, 128), 1)
    total = jnp.sum(tokens_f, axis=1, keepdims=True)
    squares = jnp.sum(tokens_f * tokens_f, axis=1, keepdims=True)
    stats[...] = jnp.transpose(jnp.where(lane == 0, total, jnp.where(lane == 1, squares, 0.0)))[0:8]
    for k in range(feat // rows):
        stats[pl.ds(2 + k, 1)] = gain[pl.ds(k * rows, rows)][None, :]

    pl.semaphore_wait(barrier, 23 - straight.astype(jnp.int32))

    stat_r = sems("r", 16)
    stat_s = sems("s", 16)

    def stat_copy(n):
        dl, dz, dc = readers[n]
        return pltpu.make_async_remote_copy(
            src_ref=stats, dst_ref=statbuf.at[H, dl, dz], send_sem=send_sem.at[stat_s + n],
            recv_sem=recv_sem.at[stat_r + 8 * H + 4 * dl + dz], device_id=reader(dl, dz, dc), device_id_type=MESH,
        )

    for n, r in enumerate(readers):
        unless(straight, r == (0, 0, 0), lambda: stat_copy(n).start())

    x_r = sems("r", 2)
    x_s = sems("s", 2)

    def token_copy(b):
        return pltpu.make_async_remote_copy(
            src_ref=tok, dst_ref=xraw.at[L], send_sem=send_sem.at[x_s + b], recv_sem=recv_sem.at[x_r + L],
            device_id={"H": C, "L": b, "C": H}, device_id_type=MESH,
        )

    for b in (1 - L, L):
        mine = jnp.logical_and(straight, L == b)

        @pl.when(jnp.logical_not(mine))
        def _():
            token_copy(b).start()

    send_w1(0, near[0])

    @pl.when(straight)
    def _():
        xraw[L] = tok[...]
        statbuf[H, 0, 0] = stats[...]

    yp_r, ym_r, ya_r, yb_r, sib_r = sems("r", 4), sems("r", 4), sems("r", 2), sems("r", 2), sems("r", 8)
    first, second = pl.ds(0, half), pl.ds(half, half)

    def to_sib(rel, b):
        copy(xbuf.at[C, rel, b], xbuf.at[C, rel, b], sib_r + 2 * rel + b, sib)

    early = lax.rem(L + swapped, 2)

    def start_y(b):
        mine = jnp.logical_and(straight, L == b)
        dl = lax.rem(L + b, 2)

        @pl.when(jnp.logical_not(mine))
        def _():
            arrive(statbuf.at[H, dl, 0], stat_r + 8 * H + 4 * dl)

        arrive(statbuf.at[1 - H, dl, 0], stat_r + 8 * (1 - H) + 4 * dl)
        for src in range(2):
            for dz in range(1, 4):
                arrive(statbuf.at[src, dl, dz], stat_r + 8 * src + 4 * dl + dz)
        summed = statbuf[0, dl, 0]
        for src, dz in [(0, 1), (0, 2), (0, 3), (1, 0), (1, 1), (1, 2), (1, 3)]:
            summed = summed + statbuf[src, dl, dz]
        column = jnp.transpose(jnp.concatenate([summed] * 16, axis=0))
        mean = column[:, 0:1] / width
        spread = column[:, 1:2] / width - mean * mean
        scale = lax.rsqrt(spread + EPS)
        gains = jnp.concatenate([statbuf[C, dl, 0, pl.ds(2 + k, 1)] for k in range(feat // rows)], axis=1)

        @pl.when(jnp.logical_not(mine))
        def _():
            arrive(xraw.at[b], x_r + b)

        xbuf[C, 0, b] = ((xraw[b].astype(F32) - mean) * scale * gains).astype(BF16)
        copy(xbuf.at[C, 0, b, first], xbuf.at[C, 3, b, first], yp_r + 2 * b, up)
        copy(xbuf.at[C, 0, b, second], xbuf.at[C, 1, b, second], ym_r + 2 * b + 1, down)
        copy(xbuf.at[C, 0, b, second], xbuf.at[C, 3, b, second], yp_r + 2 * b + 1, up)
        copy(xbuf.at[C, 0, b, first], xbuf.at[C, 1, b, first], ym_r + 2 * b, down)
        to_sib(0, b)

    def relay_y(b):
        arrive(xbuf.at[C, 3, b, first], yp_r + 2 * b)
        copy(xbuf.at[C, 3, b, first], xbuf.at[C, 2, b, first], ya_r + b, up)
        arrive(xbuf.at[C, 1, b, second], ym_r + 2 * b + 1)
        copy(xbuf.at[C, 1, b, second], xbuf.at[C, 2, b, second], yb_r + b, down)
        arrive(xbuf.at[C, 3, b, second], yp_r + 2 * b + 1)
        to_sib(3, b)
        arrive(xbuf.at[C, 1, b, first], ym_r + 2 * b)
        to_sib(1, b)

    def far_y(b):
        arrive(xbuf.at[C, 2, b, first], ya_r + b)
        arrive(xbuf.at[C, 2, b, second], yb_r + b)
        to_sib(2, b)

    start_y(early)
    start_y(1 - early)
    send_w1(0, near[1])
    for j in range(1, CHUNKS):
        for dev in near:
            send_w1(j, dev)
    for f in range(PARTS):
        for dev in near:
            send_w2(f, dev)

    items = ITEMS
    n_items = len(items)
    r1a_r, r1b_r, r2p_r, r2m_r = (sems("r", n_items) for _ in range(4))
    dp_r, dm_r, da_r, db_r = (sems("r", 8) for _ in range(4))
    e_r = sems("r", 4 * PARTS)
    zp, zm, z2 = lax.rem(Z + 1, 4), lax.rem(Z + 3, 4), lax.rem(Z + 2, 4)
    seen_w, seen_x = set(), set()

    def s1(i):
        j, rel = items[i]
        if j not in seen_w:
            seen_w.add(j)
            for src in range(2):
                arrive(w1buf.at[src, j], w1_r + src * CHUNKS + j)
        if rel not in seen_x:
            seen_x.add(rel)
            for b in range(2):
                arrive(xbuf.at[1 - C, rel, b], sib_r + 2 * rel + b)

        @pl.loop(0, 2)
        def _(b):
            acc = jnp.dot(xbuf[0, rel, b], w1buf[0, j], preferred_element_type=F32)
            acc = acc + jnp.dot(xbuf[1, rel, b], w1buf[1, j], preferred_element_type=F32)
            pbuf[i, b] = acc[:, :HEAD_DIM].astype(BF16)
            pbuf[i, 2 + b] = acc[:, HEAD_DIM:].astype(BF16)

        copy(pbuf.at[i, z2, pl.ds(0, half)], r1.at[0, i], r1a_r + i, fwd)
        copy(pbuf.at[i, z2, pl.ds(half, half)], r1.at[1, i], r1b_r + i, back)

    def s2(i):
        arrive(r1.at[0, i], r1a_r + i)
        pbuf[i, zp, pl.ds(0, half)] = (pbuf[i, zp, pl.ds(0, half)].astype(F32) + r1[0, i].astype(F32)).astype(BF16)
        copy(pbuf.at[i, zp], r2.at[0, i], r2p_r + i, fwd)
        arrive(r1.at[1, i], r1b_r + i)
        pbuf[i, zm, pl.ds(half, half)] = (
            pbuf[i, zm, pl.ds(half, half)].astype(F32) + r1[1, i].astype(F32)
        ).astype(BF16)
        copy(pbuf.at[i, zm], r2.at[1, i], r2m_r + i, back)

    def s3(i):
        j, rel = items[i]
        arrive(r2.at[0, i], r2p_r + i)
        arrive(r2.at[1, i], r2m_r + i)
        whole = (pbuf[i, Z].astype(F32) + r2[0, i].astype(F32) + r2[1, i].astype(F32)).astype(BF16)
        if j < 3:
            qkv[rel, j] = whole
        if j == 2:
            query = (head_norm(qkv[rel, 0].astype(F32)) * (1.0 / HEAD_DIM) ** 0.5).astype(BF16)
            keys = head_norm(qkv[rel, 1].astype(F32)).astype(BF16)
            scores = lax.dot_general(query, keys, (((1,), (1,)), ((), ())), preferred_element_type=F32)
            weights = jnp.exp(scores)
            probs = (weights / jnp.sum(weights, axis=-1, keepdims=True)).astype(BF16)
            hbuf[rel, Z, 0] = jnp.dot(probs, whole, preferred_element_type=F32).astype(BF16)
        if j >= 3:
            hbuf[rel, Z, j - 2] = gelu(whole.astype(F32)).astype(BF16)
        if j in (3, 5):
            k = (j - 3) // 2
            mine = hbuf.at[rel, Z, pl.ds(2 * k, 2)]
            copy(mine, mine, dp_r + 2 * rel + k, fwd)
            copy(mine, mine, dm_r + 2 * rel + k, back)

    def relay(i):
        j, rel = items[i]
        if j not in (3, 5):
            return
        k = (j - 3) // 2
        arrive(hbuf.at[rel, zm, pl.ds(2 * k, 2)], dp_r + 2 * rel + k)
        top = hbuf.at[rel, zm, pl.ds(2 * k, 2), pl.ds(0, half)]
        copy(top, top, da_r + 2 * rel + k, fwd)
        arrive(hbuf.at[rel, zp, pl.ds(2 * k, 2)], dm_r + 2 * rel + k)
        low = hbuf.at[rel, zp, pl.ds(2 * k, 2), pl.ds(half, half)]
        copy(low, low, db_r + 2 * rel + k, back)

    seen_w2, seen_h = set(), set()

    def e1(rel, f):
        if f not in seen_w2:
            seen_w2.add(f)
            for src in range(2):
                arrive(w2buf.at[src, f], w2_r + src * PARTS + f)
        if rel not in seen_h:
            seen_h.add(rel)
            for k in range(2):
                arrive(hbuf.at[rel, z2, pl.ds(2 * k, 2), pl.ds(0, half)], da_r + 2 * rel + k)
                arrive(hbuf.at[rel, z2, pl.ds(2 * k, 2), pl.ds(half, half)], db_r + 2 * rel + k)

        def product(side, b):
            hidden = jnp.concatenate([hbuf[rel, 2 * h + b, k] for k in range(4) for h in range(2)], axis=1)
            return jnp.dot(hidden, w2buf[side, f], preferred_element_type=F32).astype(BF16)

        @pl.loop(0, 2)
        def _(b):
            osend[rel, f, b] = product(1 - C, b)

        copy(osend.at[rel, f], osib.at[rel, f], e_r + rel * PARTS + f, sib)

        @pl.loop(0, 2)
        def _(b):
            obuf[rel, f, b] = product(C, b)

    ry_r = sems("r", 4 * PARTS)
    xr_r = sems("r", 2 * PARTS)
    xr_s = sems("s", 2 * PARTS)

    def final_copy(b, f):
        return pltpu.make_async_remote_copy(
            src_ref=xsend.at[f, b], dst_ref=xrecv.at[f, L], send_sem=send_sem.at[xr_s + 2 * f + b],
            recv_sem=recv_sem.at[xr_r + 2 * f + L], device_id={"H": C, "L": b, "C": H}, device_id_type=MESH,
        )

    def e2(rel, f):
        arrive(osib.at[rel, f], e_r + rel * PARTS + f)
        ry = ry_r + 4 * f
        for b in range(2):
            total = obuf[rel, f, b].astype(F32) + osib[rel, f, b].astype(F32)
            if rel == 1 and b == 0:
                arrive(ry1.at[f, 0], ry)
                total = total + ry1[f, 0].astype(F32)
            if rel == 3 and b == 1:
                arrive(ry1.at[f, 1], ry + 1)
                total = total + ry1[f, 1].astype(F32)
            if rel == 0:
                if b == 0:
                    arrive(ry2.at[f, 0], ry + 2)
                    arrive(ry2.at[f, 1], ry + 3)
                xsend[f, b] = (total + ry2[f, 0, b].astype(F32) + ry2[f, 1, b].astype(F32)).astype(BF16)
                mine = jnp.logical_and(C == H, L == b)

                @pl.when(mine)
                def _():
                    xrecv[f, b] = xsend[f, b]

                @pl.when(jnp.logical_not(mine))
                def _():
                    final_copy(b, f).start()
            else:
                obuf[rel, f, b] = total.astype(BF16)
        if rel == 2:
            copy(obuf.at[2, f, 0], ry1.at[f, 0], ry, up)
            copy(obuf.at[2, f, 1], ry1.at[f, 1], ry + 1, down)
        if rel == 1:
            copy(obuf.at[1, f], ry2.at[f, 0], ry + 2, up)
        if rel == 3:
            copy(obuf.at[3, f], ry2.at[f, 1], ry + 3, down)

    for t in range(max(n_items + LAGS[2], OUT_STEPS[-1][0] + 1)):
        if t == 0:
            relay_y(early)
        if t == 2:
            relay_y(1 - early)
        if t == FAR_STEP:
            far_y(early)
            far_y(1 - early)
        for lag, stage in zip((0, *LAGS), (s1, s2, s3, relay)):
            if 0 <= t - lag < n_items:
                stage(t - lag)
        for step, stage, rel, f in OUT_STEPS:
            if step == t and stage == 1:
                e1(rel, f)
            if step == t and stage == 2:
                e2(rel, f)

    for f in range(PARTS):
        for b in range(2):

            @pl.when(jnp.logical_not(jnp.logical_and(C == H, L == b)))
            def _():
                arrive(xrecv.at[f, b], xr_r + 2 * f + b)

        columns = pl.ds(f * WIDE, WIDE)
        out[:, columns] = (
            tok[:, columns].astype(F32) + xrecv[f, 0].astype(F32) + xrecv[f, 1].astype(F32)
        ).astype(BF16)

    for n, r in enumerate(readers):
        unless(straight, r == (0, 0, 0), lambda: stat_copy(n).wait_send())
    for d in pending:
        d.wait_send()
    for b in range(2):

        @pl.when(jnp.logical_not(jnp.logical_and(C == H, L == b)))
        def _():
            token_copy(b).wait_send()

        @pl.when(jnp.logical_not(jnp.logical_and(C == H, L == b)))
        def _():
            for f in range(PARTS):
                final_copy(b, f).wait_send()

    assert count["s"] <= N_SEND and count["r"] <= N_RECV, count


def local(tokens, norm_gain, w_qkv, w_up, w_attn_out, w_down):
    rows, feat = tokens.shape
    width = feat * lax.axis_size("H") * lax.axis_size("Z")
    n_items = len(ITEMS)
    half = rows // 2
    vmem = pltpu.VMEM
    out_part = (PARTS, 2, rows, WIDE)
    scratch = [
        vmem((8, rows), F32),
        vmem((2, 2, 4, 8, rows), F32),
        vmem((2, rows, feat), BF16),
        vmem((2, 4, 2, rows, feat), BF16),
        vmem((2, CHUNKS, feat, WIDE), BF16),
        vmem((2, PARTS, w_attn_out.shape[0] + w_down.shape[0], WIDE), BF16),
        vmem((n_items, 4, rows, HEAD_DIM), BF16),
        vmem((2, n_items, half, HEAD_DIM), BF16),
        vmem((2, n_items, rows, HEAD_DIM), BF16),
        vmem((4, 3, rows, HEAD_DIM), BF16),
        vmem((4, 4, 4, rows, HEAD_DIM), BF16),
        vmem((4, *out_part), BF16),
        vmem((4, *out_part), BF16),
        vmem((4, *out_part), BF16),
        vmem((PARTS, 2, rows, WIDE), BF16),
        vmem((PARTS, 2, 2, rows, WIDE), BF16),
        vmem(out_part, BF16),
        vmem(out_part, BF16),
        pltpu.SemaphoreType.DMA((N_SEND,)),
        pltpu.SemaphoreType.DMA((N_RECV,)),
    ]
    in_vmem = pl.BlockSpec(memory_space=pltpu.VMEM)
    anywhere = pl.BlockSpec(memory_space=pl.ANY)
    return pl.pallas_call(
        functools.partial(kernel, width),
        out_shape=jax.ShapeDtypeStruct((rows, feat), BF16),
        in_specs=[in_vmem] * 2 + [anywhere] * 4,
        out_specs=in_vmem,
        scratch_shapes=scratch,
        compiler_params=pltpu.CompilerParams(
            collective_id=0, has_side_effects=True, vmem_limit_bytes=60 * 1024 * 1024
        ),
        name="layer",
    )(tokens, norm_gain, w_qkv.transpose(1, 0, 2), w_up, w_attn_out, w_down)


def solution(mesh):
    torus = Mesh(mesh.devices.reshape(2, 4, 2, 2, 4), ("L", "Y", "C", "H", "Z"))
    in_specs = (P(DP, MP), P(MP), P(MP, None, DP), P(MP, DP), P(DP, MP), P(DP, MP))
    return jax.shard_map(local, mesh=torus, in_specs=in_specs, out_specs=P(DP, MP), check_vma=False)
```

```python
import functools

import jax
import jax.numpy as jnp
from jax import lax
from jax.experimental import pallas as pl
from jax.experimental.pallas import tpu as pltpu
from jax.sharding import Mesh
from jax.sharding import PartitionSpec as P

HEAD_DIM = 128
PATCHES = 256
EPS = 1e-06
MESH = pl.DeviceIdType.MESH
F32 = jnp.float32
BF16 = jnp.bfloat16
DP = ("L", "Y", "C")
MP = ("H", "Z")

CHUNKS = 6
WIDE = 2 * HEAD_DIM
PARTS = 3
ORDER = (
    ("y1", 0, 0), ("s1", 0, 0), ("y2", 0, 0), ("s2", 0, 0), ("s3", 0, 0), ("s1", 1, 0), ("s1", 0, 1), ("s1", 1, 1),
    ("s1", 0, 3), ("s1", 1, 3), ("s2", 1, 0), ("s2", 0, 1), ("s2", 1, 1), ("y3", 0, 0), ("s2", 0, 3), ("s2", 1, 3),
    ("s3", 1, 0), ("s3", 0, 1), ("s1", 2, 1), ("s3", 1, 1), ("s1", 0, 2), ("s3", 0, 3), ("s1", 1, 2), ("s1", 2, 2),
    ("s3", 1, 3), ("s1", 2, 3), ("s2", 2, 1), ("s2", 0, 2), ("s2", 1, 2), ("s2", 2, 2), ("s2", 2, 3), ("s3", 2, 1),
    ("s3", 0, 2), ("s1", 3, 1), ("s3", 1, 2), ("s1", 3, 2), ("s3", 2, 2), ("s1", 3, 3), ("s3", 2, 3), ("s2", 3, 1),
    ("s1", 4, 1), ("s2", 3, 2), ("s2", 3, 3), ("s3", 3, 1), ("s2", 4, 1), ("s3", 3, 2), ("s3", 3, 3), ("s4", 0, 1),
    ("s3", 4, 1), ("s4", 0, 2), ("s1", 5, 1), ("s4", 0, 3), ("s1", 4, 2), ("s1", 5, 2), ("s2", 5, 1), ("s1", 4, 3),
    ("s2", 4, 2), ("s2", 5, 2), ("s3", 5, 1), ("s2", 4, 3), ("s3", 4, 2), ("s3", 5, 2), ("s4", 1, 1), ("s3", 4, 3),
    ("s1", 2, 0), ("s1", 5, 3), ("s4", 1, 2), ("e1", 0, 1), ("e1", 1, 1), ("s2", 2, 0), ("s2", 5, 3), ("e1", 0, 2),
    ("e1", 2, 1), ("e1", 1, 2), ("e2", 0, 2), ("s3", 2, 0), ("s3", 5, 3), ("e1", 2, 2), ("e2", 1, 2), ("s1", 3, 0),
    ("e2", 2, 2), ("s1", 4, 0), ("s1", 5, 0), ("e2", 0, 1), ("s4", 1, 3), ("s2", 3, 0), ("s2", 4, 0), ("e2", 1, 1),
    ("s2", 5, 0), ("e1", 0, 3), ("e2", 2, 1), ("s3", 3, 0), ("e1", 1, 3), ("s3", 4, 0), ("e2", 0, 3), ("e1", 2, 3),
    ("s3", 5, 0), ("e2", 1, 3), ("e2", 2, 3), ("s4", 0, 0), ("s4", 1, 0), ("e1", 0, 0), ("e1", 1, 0), ("e1", 2, 0),
    ("e2", 0, 0), ("e2", 1, 0), ("e2", 2, 0),
)
N_SEND = 224
N_RECV = 224


def gelu(u):
    return 0.5 * u * (1.0 + jnp.tanh(0.7978845608028654 * (u + 0.044715 * (u * u * u))))


def head_norm(values):
    mean = jnp.mean(values, axis=-1, keepdims=True)
    centered = values - mean
    spread = jnp.mean(centered * centered, axis=-1, keepdims=True)
    return centered * lax.rsqrt(spread + EPS)


def kernel(
    width,
    tok, gain, w_qkv, w_up, w_attn, w_down,
    out,
    stats, statbuf, xraw, xbuf, w1buf, w2buf, pbuf, r1, r2, qkv, hbuf, obuf, osend, osib, ry1, ry2, xsend, xrecv,
    send_sem, recv_sem,
):
    L, Y, C, H, Z = (lax.axis_index(a) for a in ("L", "Y", "C", "H", "Z"))
    rows, feat = tok.shape
    half = rows // 2
    near = ({"L": 1 - L, "H": C}, {"L": 1 - L, "H": 1 - C})
    up, down = {"Y": lax.rem(Y + 1, 4)}, {"Y": lax.rem(Y + 3, 4)}
    fwd, back = {"Z": lax.rem(Z + 1, 4)}, {"Z": lax.rem(Z + 3, 4)}
    sib = {"C": 1 - C}
    swapped = (C != H).astype(jnp.int32)
    straight = C == H

    count = {"s": 0, "r": 0}
    pending = []

    def sems(kind, n=1):
        first = count[kind]
        count[kind] += n
        return first

    def copy(src, dst, recv, dev):
        d = pltpu.make_async_remote_copy(
            src_ref=src, dst_ref=dst, send_sem=send_sem.at[sems("s")], recv_sem=recv_sem.at[recv],
            device_id=dev, device_id_type=MESH,
        )
        d.start()
        pending.append(d)

    def arrive(dst, recv):
        pltpu.make_async_remote_copy(
            src_ref=dst, dst_ref=dst, send_sem=send_sem.at[0], recv_sem=recv_sem.at[recv],
            device_id=sib, device_id_type=MESH,
        ).wait_recv()

    barrier = pltpu.get_barrier_semaphore()
    for dev in (*near, up, down, fwd, back, sib):
        pl.semaphore_signal(barrier, inc=1, device_id=dev, device_id_type=MESH)

    readers = [(dl, dz, dc) for dl in range(2) for dz in range(4) for dc in range(2)]

    def reader(dl, dz, dc):
        return {"H": C, "L": lax.rem(L + dl, 2), "Z": lax.rem(Z + dz, 4), "C": lax.rem(C + dc, 2)}

    def unless(condition, skip, f):
        if skip:
            pl.when(jnp.logical_not(condition))(f)
        else:
            f()

    for dh, dl, dz in [(dh, dl, dz) for dh in range(2) for dl in range(2) for dz in range(4)]:

        def greet():
            source = {"C": H, "H": lax.rem(H + dh, 2), "L": lax.rem(L + dl, 2), "Z": lax.rem(Z + dz, 4)}
            pl.semaphore_signal(barrier, inc=1, device_id=source, device_id_type=MESH)

        unless(straight, dh + dl + dz == 0, greet)

    w1_r = sems("r", 2 * CHUNKS)
    w2_r = sems("r", 2 * PARTS)

    def send_w1(j, dev):
        block = w_qkv.at[j] if j < 3 else w_up.at[:, pl.ds((j - 3) * WIDE, WIDE)]
        copy(block, w1buf.at[H, j], w1_r + H * CHUNKS + j, dev)

    def send_w2(f, dev):
        top, columns = w_attn.shape[0], pl.ds(f * WIDE, WIDE)
        copy(w_attn.at[:, columns], w2buf.at[H, f, pl.ds(0, top)], w2_r + H * PARTS + f, dev)
        copy(w_down.at[:, columns], w2buf.at[H, f, pl.ds(top, w_down.shape[0])], w2_r + H * PARTS + f, dev)

    tokens_f = tok[...].astype(F32)
    lane = lax.broadcasted_iota(jnp.int32, (rows, 128), 1)
    total = jnp.sum(tokens_f, axis=1, keepdims=True)
    squares = jnp.sum(tokens_f * tokens_f, axis=1, keepdims=True)
    stats[...] = jnp.transpose(jnp.where(lane == 0, total, jnp.where(lane == 1, squares, 0.0)))[0:8]
    for k in range(feat // rows):
        stats[pl.ds(2 + k, 1)] = gain[pl.ds(k * rows, rows)][None, :]

    pl.semaphore_wait(barrier, 23 - straight.astype(jnp.int32))

    stat_r = sems("r", 16)
    stat_s = sems("s", 16)

    def stat_copy(n):
        dl, dz, dc = readers[n]
        return pltpu.make_async_remote_copy(
            src_ref=stats, dst_ref=statbuf.at[H, dl, dz], send_sem=send_sem.at[stat_s + n],
            recv_sem=recv_sem.at[stat_r + 8 * H + 4 * dl + dz], device_id=reader(dl, dz, dc), device_id_type=MESH,
        )

    for n, r in enumerate(readers):
        unless(straight, r == (0, 0, 0), lambda: stat_copy(n).start())

    x_r = sems("r", 4)
    x_s = sems("s", 4)

    first, second = pl.ds(0, half), pl.ds(half, half)
    halves = (first, second)

    def token_copy(b, n):
        return pltpu.make_async_remote_copy(
            src_ref=tok.at[halves[n]], dst_ref=xraw.at[L, halves[n]], send_sem=send_sem.at[x_s + 2 * b + n],
            recv_sem=recv_sem.at[x_r + 2 * L + n], device_id={"H": C, "L": b, "C": H}, device_id_type=MESH,
        )

    for b in (1 - L, L):
        mine = jnp.logical_and(straight, L == b)

        @pl.when(jnp.logical_not(mine))
        def _():
            for n in range(2):
                token_copy(b, n).start()

    send_w1(0, near[0])

    @pl.when(straight)
    def _():
        xraw[L] = tok[...]
        statbuf[H, 0, 0] = stats[...]

    yp_r, ym_r, ya_r, yb_r, sib_r = sems("r", 4), sems("r", 4), sems("r", 2), sems("r", 2), sems("r", 8)

    def to_sib(rel, b):
        copy(xbuf.at[C, rel, b], xbuf.at[C, rel, b], sib_r + 2 * rel + b, sib)

    early = lax.rem(L + swapped, 2)

    def start_y(b):
        mine = jnp.logical_and(straight, L == b)
        dl = lax.rem(L + b, 2)

        @pl.when(jnp.logical_not(mine))
        def _():
            arrive(statbuf.at[H, dl, 0], stat_r + 8 * H + 4 * dl)

        arrive(statbuf.at[1 - H, dl, 0], stat_r + 8 * (1 - H) + 4 * dl)
        for src in range(2):
            for dz in range(1, 4):
                arrive(statbuf.at[src, dl, dz], stat_r + 8 * src + 4 * dl + dz)
        summed = statbuf[0, dl, 0]
        for src, dz in [(0, 1), (0, 2), (0, 3), (1, 0), (1, 1), (1, 2), (1, 3)]:
            summed = summed + statbuf[src, dl, dz]
        column = jnp.transpose(jnp.concatenate([summed] * 16, axis=0))
        mean = column[:, 0:1] / width
        spread = column[:, 1:2] / width - mean * mean
        scale = lax.rsqrt(spread + EPS)
        gains = jnp.concatenate([statbuf[C, dl, 0, pl.ds(2 + k, 1)] for k in range(feat // rows)], axis=1)

        for n, part in enumerate(halves):

            @pl.when(jnp.logical_not(mine))
            def _():
                arrive(xraw.at[b, part], x_r + 2 * b + n)

            at = slice(n * half, (n + 1) * half)
            xbuf[C, 0, b, part] = ((xraw[b, part].astype(F32) - mean[at]) * scale[at] * gains).astype(BF16)
            copy(xbuf.at[C, 0, b, part], xbuf.at[C, 3, b, part], yp_r + 2 * b + n, up)
            copy(xbuf.at[C, 0, b, part], xbuf.at[C, 1, b, part], ym_r + 2 * b + n, down)
        to_sib(0, b)

    def relay_y(b):
        arrive(xbuf.at[C, 3, b, first], yp_r + 2 * b)
        copy(xbuf.at[C, 3, b, first], xbuf.at[C, 2, b, first], ya_r + b, up)
        arrive(xbuf.at[C, 1, b, first], ym_r + 2 * b)
        arrive(xbuf.at[C, 1, b, second], ym_r + 2 * b + 1)
        copy(xbuf.at[C, 1, b, second], xbuf.at[C, 2, b, second], yb_r + b, down)
        to_sib(1, b)
        arrive(xbuf.at[C, 3, b, second], yp_r + 2 * b + 1)
        to_sib(3, b)

    def far_y(b):
        arrive(xbuf.at[C, 2, b, first], ya_r + b)
        arrive(xbuf.at[C, 2, b, second], yb_r + b)
        to_sib(2, b)

    start_y(early)
    start_y(1 - early)
    send_w1(0, near[1])
    for j in range(1, CHUNKS):
        for dev in near:
            send_w1(j, dev)
    for f in range(PARTS):
        for dev in near:
            send_w2(f, dev)

    n_items = 4 * CHUNKS
    r1a_r, r1b_r, r2p_r, r2m_r = (sems("r", n_items) for _ in range(4))
    dp_r, dm_r, da_r, db_r = (sems("r", 8) for _ in range(4))
    e_r = sems("r", 4 * PARTS)
    zp, zm, z2 = lax.rem(Z + 1, 4), lax.rem(Z + 3, 4), lax.rem(Z + 2, 4)
    seen_w, seen_x = set(), set()

    def s1(j, rel):
        i = 4 * j + rel
        if j not in seen_w:
            seen_w.add(j)
            for src in range(2):
                arrive(w1buf.at[src, j], w1_r + src * CHUNKS + j)
        if rel not in seen_x:
            seen_x.add(rel)
            for b in range(2):
                arrive(xbuf.at[1 - C, rel, b], sib_r + 2 * rel + b)

        @pl.loop(0, 2)
        def _(b):
            acc = jnp.dot(xbuf[0, rel, b], w1buf[0, j], preferred_element_type=F32)
            acc = acc + jnp.dot(xbuf[1, rel, b], w1buf[1, j], preferred_element_type=F32)
            pbuf[i, b] = acc[:, :HEAD_DIM].astype(BF16)
            pbuf[i, 2 + b] = acc[:, HEAD_DIM:].astype(BF16)

        copy(pbuf.at[i, z2, pl.ds(0, half)], r1.at[0, i], r1a_r + i, fwd)
        copy(pbuf.at[i, z2, pl.ds(half, half)], r1.at[1, i], r1b_r + i, back)

    def s2(j, rel):
        i = 4 * j + rel
        arrive(r1.at[0, i], r1a_r + i)
        pbuf[i, zp, pl.ds(0, half)] = (pbuf[i, zp, pl.ds(0, half)].astype(F32) + r1[0, i].astype(F32)).astype(BF16)
        copy(pbuf.at[i, zp], r2.at[0, i], r2p_r + i, fwd)
        arrive(r1.at[1, i], r1b_r + i)
        pbuf[i, zm, pl.ds(half, half)] = (
            pbuf[i, zm, pl.ds(half, half)].astype(F32) + r1[1, i].astype(F32)
        ).astype(BF16)
        copy(pbuf.at[i, zm], r2.at[1, i], r2m_r + i, back)

    def s3(j, rel):
        i = 4 * j + rel
        arrive(r2.at[0, i], r2p_r + i)
        arrive(r2.at[1, i], r2m_r + i)
        whole = (pbuf[i, Z].astype(F32) + r2[0, i].astype(F32) + r2[1, i].astype(F32)).astype(BF16)
        if j < 3:
            qkv[rel, j] = whole
        if j == 2:
            query = (head_norm(qkv[rel, 0].astype(F32)) * (1.0 / HEAD_DIM) ** 0.5).astype(BF16)
            keys = head_norm(qkv[rel, 1].astype(F32)).astype(BF16)
            scores = lax.dot_general(query, keys, (((1,), (1,)), ((), ())), preferred_element_type=F32)
            weights = jnp.exp(scores)
            probs = (weights / jnp.sum(weights, axis=-1, keepdims=True)).astype(BF16)
            hbuf[rel, Z, 0] = jnp.dot(probs, whole, preferred_element_type=F32).astype(BF16)
        if j >= 3:
            hbuf[rel, Z, j - 2] = gelu(whole.astype(F32)).astype(BF16)
        if j in (3, 5):
            k = (j - 3) // 2
            mine = hbuf.at[rel, Z, pl.ds(2 * k, 2)]
            copy(mine, mine, dp_r + 2 * rel + k, fwd)
            copy(mine, mine, dm_r + 2 * rel + k, back)

    def relay(k, rel):
        arrive(hbuf.at[rel, zm, pl.ds(2 * k, 2)], dp_r + 2 * rel + k)
        top = hbuf.at[rel, zm, pl.ds(2 * k, 2), pl.ds(0, half)]
        copy(top, top, da_r + 2 * rel + k, fwd)
        arrive(hbuf.at[rel, zp, pl.ds(2 * k, 2)], dm_r + 2 * rel + k)
        low = hbuf.at[rel, zp, pl.ds(2 * k, 2), pl.ds(half, half)]
        copy(low, low, db_r + 2 * rel + k, back)

    seen_w2, seen_h = set(), set()

    def e1(f, rel):
        if f not in seen_w2:
            seen_w2.add(f)
            for src in range(2):
                arrive(w2buf.at[src, f], w2_r + src * PARTS + f)
        if rel not in seen_h:
            seen_h.add(rel)
            for k in range(2):
                arrive(hbuf.at[rel, z2, pl.ds(2 * k, 2), pl.ds(0, half)], da_r + 2 * rel + k)
                arrive(hbuf.at[rel, z2, pl.ds(2 * k, 2), pl.ds(half, half)], db_r + 2 * rel + k)

        def product(side, b):
            hidden = jnp.concatenate([hbuf[rel, 2 * h + b, k] for k in range(4) for h in range(2)], axis=1)
            return jnp.dot(hidden, w2buf[side, f], preferred_element_type=F32).astype(BF16)

        @pl.loop(0, 2)
        def _(b):
            osend[rel, f, b] = product(1 - C, b)

        copy(osend.at[rel, f], osib.at[rel, f], e_r + rel * PARTS + f, sib)

        @pl.loop(0, 2)
        def _(b):
            obuf[rel, f, b] = product(C, b)

    ry_r = sems("r", 4 * PARTS)
    xr_r = sems("r", 2 * PARTS)
    xr_s = sems("s", 2 * PARTS)

    def final_copy(b, f):
        return pltpu.make_async_remote_copy(
            src_ref=xsend.at[f, b], dst_ref=xrecv.at[f, L], send_sem=send_sem.at[xr_s + 2 * f + b],
            recv_sem=recv_sem.at[xr_r + 2 * f + L], device_id={"H": C, "L": b, "C": H}, device_id_type=MESH,
        )

    def e2(f, rel):
        arrive(osib.at[rel, f], e_r + rel * PARTS + f)
        ry = ry_r + 4 * f
        for b in range(2):
            total = obuf[rel, f, b].astype(F32) + osib[rel, f, b].astype(F32)
            if rel == 1 and b == 0:
                arrive(ry1.at[f, 0], ry)
                total = total + ry1[f, 0].astype(F32)
            if rel == 3 and b == 1:
                arrive(ry1.at[f, 1], ry + 1)
                total = total + ry1[f, 1].astype(F32)
            if rel == 0:
                if b == 0:
                    arrive(ry2.at[f, 0], ry + 2)
                    arrive(ry2.at[f, 1], ry + 3)
                xsend[f, b] = (total + ry2[f, 0, b].astype(F32) + ry2[f, 1, b].astype(F32)).astype(BF16)
                mine = jnp.logical_and(C == H, L == b)

                @pl.when(mine)
                def _():
                    xrecv[f, b] = xsend[f, b]

                @pl.when(jnp.logical_not(mine))
                def _():
                    final_copy(b, f).start()
            else:
                obuf[rel, f, b] = total.astype(BF16)
        if rel == 2:
            copy(obuf.at[2, f, 0], ry1.at[f, 0], ry, up)
            copy(obuf.at[2, f, 1], ry1.at[f, 1], ry + 1, down)
        if rel == 1:
            copy(obuf.at[1, f], ry2.at[f, 0], ry + 2, up)
        if rel == 3:
            copy(obuf.at[3, f], ry2.at[f, 1], ry + 3, down)

    stages = {
        "y1": lambda a, rel: relay_y(early),
        "y2": lambda a, rel: relay_y(1 - early),
        "y3": lambda a, rel: (far_y(early), far_y(1 - early)),
        "s1": s1, "s2": s2, "s3": s3, "s4": relay, "e1": e1, "e2": e2,
    }
    for stage, a, rel in ORDER:
        stages[stage](a, rel)

    for f in range(PARTS):
        for b in range(2):

            @pl.when(jnp.logical_not(jnp.logical_and(C == H, L == b)))
            def _():
                arrive(xrecv.at[f, b], xr_r + 2 * f + b)

        columns = pl.ds(f * WIDE, WIDE)
        out[:, columns] = (
            tok[:, columns].astype(F32) + xrecv[f, 0].astype(F32) + xrecv[f, 1].astype(F32)
        ).astype(BF16)

    for n, r in enumerate(readers):
        unless(straight, r == (0, 0, 0), lambda: stat_copy(n).wait_send())
    for d in pending:
        d.wait_send()
    for b in range(2):

        @pl.when(jnp.logical_not(jnp.logical_and(C == H, L == b)))
        def _():
            for n in range(2):
                token_copy(b, n).wait_send()

        @pl.when(jnp.logical_not(jnp.logical_and(C == H, L == b)))
        def _():
            for f in range(PARTS):
                final_copy(b, f).wait_send()

    assert count["s"] <= N_SEND and count["r"] <= N_RECV, count


def local(tokens, norm_gain, w_qkv, w_up, w_attn_out, w_down):
    rows, feat = tokens.shape
    width = feat * lax.axis_size("H") * lax.axis_size("Z")
    n_items = 4 * CHUNKS
    half = rows // 2
    vmem = pltpu.VMEM
    out_part = (PARTS, 2, rows, WIDE)
    scratch = [
        vmem((8, rows), F32),
        vmem((2, 2, 4, 8, rows), F32),
        vmem((2, rows, feat), BF16),
        vmem((2, 4, 2, rows, feat), BF16),
        vmem((2, CHUNKS, feat, WIDE), BF16),
        vmem((2, PARTS, w_attn_out.shape[0] + w_down.shape[0], WIDE), BF16),
        vmem((n_items, 4, rows, HEAD_DIM), BF16),
        vmem((2, n_items, half, HEAD_DIM), BF16),
        vmem((2, n_items, rows, HEAD_DIM), BF16),
        vmem((4, 3, rows, HEAD_DIM), BF16),
        vmem((4, 4, 4, rows, HEAD_DIM), BF16),
        vmem((4, *out_part), BF16),
        vmem((4, *out_part), BF16),
        vmem((4, *out_part), BF16),
        vmem((PARTS, 2, rows, WIDE), BF16),
        vmem((PARTS, 2, 2, rows, WIDE), BF16),
        vmem(out_part, BF16),
        vmem(out_part, BF16),
        pltpu.SemaphoreType.DMA((N_SEND,)),
        pltpu.SemaphoreType.DMA((N_RECV,)),
    ]
    in_vmem = pl.BlockSpec(memory_space=pltpu.VMEM)
    anywhere = pl.BlockSpec(memory_space=pl.ANY)
    return pl.pallas_call(
        functools.partial(kernel, width),
        out_shape=jax.ShapeDtypeStruct((rows, feat), BF16),
        in_specs=[in_vmem] * 2 + [anywhere] * 4,
        out_specs=in_vmem,
        scratch_shapes=scratch,
        compiler_params=pltpu.CompilerParams(
            collective_id=0, has_side_effects=True, vmem_limit_bytes=60 * 1024 * 1024
        ),
        name="layer",
    )(tokens, norm_gain, w_qkv.transpose(1, 0, 2), w_up, w_attn_out, w_down)


def solution(mesh):
    torus = Mesh(mesh.devices.reshape(2, 4, 2, 2, 4), ("L", "Y", "C", "H", "Z"))
    in_specs = (P(DP, MP), P(MP), P(MP, None, DP), P(MP, DP), P(DP, MP), P(DP, MP))
    return jax.shard_map(local, mesh=torus, in_specs=in_specs, out_specs=P(DP, MP), check_vma=False)
```

```python
import functools
import math

import jax
import jax.numpy as jnp
from jax import lax
from jax.experimental import pallas as pl
from jax.experimental.pallas import tpu as pltpu
from jax.sharding import Mesh
from jax.sharding import PartitionSpec as P

HEAD_DIM = 128
PATCHES = 256
EPS = 1e-06
MESH = pl.DeviceIdType.MESH
F32 = jnp.float32
BF16 = jnp.bfloat16
DP = ("L", "Y", "C")
MP = ("H", "Z")

CHUNKS = 6
WIDE = 2 * HEAD_DIM
PARTS = 3
ORDER = (
    ("y1", 0, 0), ("s1", 0, 0), ("y2", 0, 0), ("s2", 0, 0), ("s3", 0, 0), ("s1", 1, 0), ("s1", 0, 1), ("s1", 1, 1),
    ("s1", 0, 3), ("s1", 1, 3), ("s2", 1, 0), ("s2", 0, 1), ("s2", 1, 1), ("y3", 0, 0), ("s2", 0, 3), ("s2", 1, 3),
    ("s3", 1, 0), ("s3", 0, 1), ("s1", 2, 1), ("s3", 1, 1), ("s1", 0, 2), ("s3", 0, 3), ("s1", 1, 2), ("s1", 2, 2),
    ("s3", 1, 3), ("s1", 2, 3), ("s2", 2, 1), ("s2", 0, 2), ("s2", 1, 2), ("s2", 2, 2), ("s2", 2, 3), ("s3", 2, 1),
    ("s3", 0, 2), ("s1", 3, 1), ("s3", 1, 2), ("s1", 3, 2), ("s3", 2, 2), ("s1", 3, 3), ("s3", 2, 3), ("s2", 3, 1),
    ("s1", 4, 1), ("s2", 3, 2), ("s2", 3, 3), ("s3", 3, 1), ("s2", 4, 1), ("s3", 3, 2), ("s3", 3, 3), ("s4", 0, 1),
    ("s3", 4, 1), ("s4", 0, 2), ("s1", 5, 1), ("s4", 0, 3), ("s1", 4, 2), ("s1", 5, 2), ("s2", 5, 1), ("s1", 4, 3),
    ("s2", 4, 2), ("s2", 5, 2), ("s3", 5, 1), ("s2", 4, 3), ("s3", 4, 2), ("s3", 5, 2), ("s4", 1, 1), ("s3", 4, 3),
    ("s1", 2, 0), ("s1", 5, 3), ("s4", 1, 2), ("e1", 0, 1), ("e1", 1, 1), ("s2", 2, 0), ("s2", 5, 3), ("e1", 0, 2),
    ("e1", 2, 1), ("e1", 1, 2), ("e2", 0, 2), ("s3", 2, 0), ("s3", 5, 3), ("e1", 2, 2), ("e2", 1, 2), ("s1", 3, 0),
    ("e2", 2, 2), ("s1", 4, 0), ("s1", 5, 0), ("e2", 0, 1), ("s4", 1, 3), ("s2", 3, 0), ("s2", 4, 0), ("e2", 1, 1),
    ("s2", 5, 0), ("e1", 0, 3), ("e2", 2, 1), ("s3", 3, 0), ("e1", 1, 3), ("s3", 4, 0), ("e2", 0, 3), ("e1", 2, 3),
    ("s3", 5, 0), ("e2", 1, 3), ("e2", 2, 3), ("s4", 0, 0), ("s4", 1, 0), ("e1", 0, 0), ("e1", 1, 0), ("e1", 2, 0),
    ("e2", 0, 0), ("e2", 1, 0), ("e2", 2, 0),
)
N_SEND = 37
N_RECV = 129


def gelu(u):
    return 0.5 * u * (1.0 + jnp.tanh(0.7978845608028654 * (u + 0.044715 * (u * u * u))))


def head_norm(values):
    mean = jnp.mean(values, axis=-1, keepdims=True)
    centered = values - mean
    spread = jnp.mean(centered * centered, axis=-1, keepdims=True)
    return centered * lax.rsqrt(spread + EPS)


def kernel(
    width,
    tok, gain, w_qkv, w_up, w_attn, w_down,
    out,
    stats, statbuf, xraw, xbuf, w1buf, w2buf, pbuf, r1, r2, qkv, hbuf, oall, osib, ry1, ry2, xsend, xrecv,
    send_sem, recv_sem,
):
    L, Y, C, H, Z = (lax.axis_index(a) for a in ("L", "Y", "C", "H", "Z"))
    rows, feat = tok.shape
    half = rows // 2
    near = ({"L": 1 - L, "H": C}, {"L": 1 - L, "H": 1 - C})
    up, down = {"Y": lax.rem(Y + 1, 4)}, {"Y": lax.rem(Y + 3, 4)}
    fwd, back = {"Z": lax.rem(Z + 1, 4)}, {"Z": lax.rem(Z + 3, 4)}
    sib = {"C": 1 - C}
    swapped = (C != H).astype(jnp.int32)
    straight = C == H

    count = {"s": 0, "r": 0}
    pending = {}

    def sems(kind, n=1):
        first = count[kind]
        count[kind] += n
        return first

    def size(ref):
        return math.prod(ref.shape) * 2

    def copy(src, dst, recv, dev, kind):
        if kind not in pending:
            pending[kind] = [sems("s"), 0]
        pending[kind][1] += size(src)
        pltpu.make_async_remote_copy(
            src_ref=src, dst_ref=dst, send_sem=send_sem.at[pending[kind][0]], recv_sem=recv_sem.at[recv],
            device_id=dev, device_id_type=MESH,
        ).start()

    def arrive(dst, recv):
        pltpu.make_async_remote_copy(
            src_ref=dst, dst_ref=dst, send_sem=send_sem.at[0], recv_sem=recv_sem.at[recv],
            device_id=sib, device_id_type=MESH,
        ).wait_recv()

    barrier = pltpu.get_barrier_semaphore()
    for dev in (*near, up, down, fwd, back, sib):
        pl.semaphore_signal(barrier, inc=1, device_id=dev, device_id_type=MESH)

    readers = [(dl, dz, dc) for dl in range(2) for dz in range(4) for dc in range(2)]

    def reader(dl, dz, dc):
        return {"H": C, "L": lax.rem(L + dl, 2), "Z": lax.rem(Z + dz, 4), "C": lax.rem(C + dc, 2)}

    def unless(condition, skip, f):
        if skip:
            pl.when(jnp.logical_not(condition))(f)
        else:
            f()

    for dh, dl, dz in [(dh, dl, dz) for dh in range(2) for dl in range(2) for dz in range(4)]:

        def greet():
            source = {"C": H, "H": lax.rem(H + dh, 2), "L": lax.rem(L + dl, 2), "Z": lax.rem(Z + dz, 4)}
            pl.semaphore_signal(barrier, inc=1, device_id=source, device_id_type=MESH)

        unless(straight, dh + dl + dz == 0, greet)

    w1_r = sems("r", CHUNKS)
    w2_r = sems("r", PARTS)

    def send_w1(j, dev):
        block = w_qkv.at[j] if j < 3 else w_up.at[:, pl.ds((j - 3) * WIDE, WIDE)]
        copy(block, w1buf.at[j, H], w1_r + j, dev, "w1")

    def send_w2(f, dev):
        top, columns = w_attn.shape[0], pl.ds(f * WIDE, WIDE)
        copy(w_attn.at[:, columns], w2buf.at[H, f, pl.ds(0, top)], w2_r + f, dev, "w2")
        copy(w_down.at[:, columns], w2buf.at[H, f, pl.ds(top, w_down.shape[0])], w2_r + f, dev, "w2")

    tokens_f = tok[...].astype(F32)
    lane = lax.broadcasted_iota(jnp.int32, (rows, 128), 1)
    total = jnp.sum(tokens_f, axis=1, keepdims=True)
    squares = jnp.sum(tokens_f * tokens_f, axis=1, keepdims=True)
    stats[...] = jnp.transpose(jnp.where(lane == 0, total, jnp.where(lane == 1, squares, 0.0)))[0:8]
    for k in range(feat // rows):
        stats[pl.ds(2 + k, 1)] = gain[pl.ds(k * rows, rows)][None, :]

    pl.semaphore_wait(barrier, 23 - straight.astype(jnp.int32))

    stat_r = sems("r", 16)
    stat_s = sems("s", 16)

    def stat_copy(n):
        dl, dz, dc = readers[n]
        return pltpu.make_async_remote_copy(
            src_ref=stats, dst_ref=statbuf.at[H, dl, dz], send_sem=send_sem.at[stat_s + n],
            recv_sem=recv_sem.at[stat_r + 8 * H + 4 * dl + dz], device_id=reader(dl, dz, dc), device_id_type=MESH,
        )

    for n, r in enumerate(readers):
        unless(straight, r == (0, 0, 0), lambda: stat_copy(n).start())

    x_r = sems("r", 4)
    x_s = sems("s", 4)

    first, second = pl.ds(0, half), pl.ds(half, half)
    halves = (first, second)

    def token_copy(b, n):
        return pltpu.make_async_remote_copy(
            src_ref=tok.at[halves[n]], dst_ref=xraw.at[L, halves[n]], send_sem=send_sem.at[x_s + 2 * b + n],
            recv_sem=recv_sem.at[x_r + 2 * L + n], device_id={"H": C, "L": b, "C": H}, device_id_type=MESH,
        )

    for b in (1 - L, L):
        mine = jnp.logical_and(straight, L == b)

        @pl.when(jnp.logical_not(mine))
        def _():
            for n in range(2):
                token_copy(b, n).start()

    send_w1(0, near[0])

    @pl.when(straight)
    def _():
        xraw[L] = tok[...]
        statbuf[H, 0, 0] = stats[...]

    yp_r, ym_r, far_r, sib_r = sems("r", 4), sems("r", 4), sems("r"), sems("r", 4)

    def to_sib(rel, b):
        copy(xbuf.at[C, rel, b], xbuf.at[C, rel, b], sib_r + rel, sib, "core")

    early = lax.rem(L + swapped, 2)

    def start_y(b):
        mine = jnp.logical_and(straight, L == b)
        dl = lax.rem(L + b, 2)

        @pl.when(jnp.logical_not(mine))
        def _():
            arrive(statbuf.at[H, dl, 0], stat_r + 8 * H + 4 * dl)

        arrive(statbuf.at[1 - H, dl, 0], stat_r + 8 * (1 - H) + 4 * dl)
        for src in range(2):
            for dz in range(1, 4):
                arrive(statbuf.at[src, dl, dz], stat_r + 8 * src + 4 * dl + dz)
        summed = statbuf[0, dl, 0]
        for src, dz in [(0, 1), (0, 2), (0, 3), (1, 0), (1, 1), (1, 2), (1, 3)]:
            summed = summed + statbuf[src, dl, dz]
        column = jnp.transpose(jnp.concatenate([summed] * 16, axis=0))
        mean = column[:, 0:1] / width
        spread = column[:, 1:2] / width - mean * mean
        scale = lax.rsqrt(spread + EPS)
        gains = jnp.concatenate([statbuf[C, dl, 0, pl.ds(2 + k, 1)] for k in range(feat // rows)], axis=1)

        for n, part in enumerate(halves):

            @pl.when(jnp.logical_not(mine))
            def _():
                arrive(xraw.at[b, part], x_r + 2 * b + n)

            at = slice(n * half, (n + 1) * half)
            xbuf[C, 0, b, part] = ((xraw[b, part].astype(F32) - mean[at]) * scale[at] * gains).astype(BF16)
            copy(xbuf.at[C, 0, b, part], xbuf.at[C, 3, b, part], yp_r + 2 * b + n, up, "y")
            copy(xbuf.at[C, 0, b, part], xbuf.at[C, 1, b, part], ym_r + 2 * b + n, down, "y")
        to_sib(0, b)

    def relay_y(b):
        arrive(xbuf.at[C, 3, b, first], yp_r + 2 * b)
        copy(xbuf.at[C, 3, b, first], xbuf.at[C, 2, b, first], far_r, up, "y")
        arrive(xbuf.at[C, 1, b, first], ym_r + 2 * b)
        arrive(xbuf.at[C, 1, b, second], ym_r + 2 * b + 1)
        copy(xbuf.at[C, 1, b, second], xbuf.at[C, 2, b, second], far_r, down, "y")
        to_sib(1, b)
        arrive(xbuf.at[C, 3, b, second], yp_r + 2 * b + 1)
        to_sib(3, b)

    def far_y():
        arrive(xbuf.at[C, 2], far_r)
        for b in range(2):
            to_sib(2, b)

    start_y(early)
    start_y(1 - early)
    send_w1(0, near[1])
    for j in range(1, CHUNKS):
        for dev in near:
            send_w1(j, dev)
    for f in range(PARTS):
        for dev in near:
            send_w2(f, dev)

    n_items = 4 * CHUNKS
    r1_r, r2_r = sems("r", n_items), sems("r", n_items)
    near_r, far_h = sems("r", 8), sems("r", 4)
    e_r = sems("r", 4 * PARTS)
    zp, zm, z2 = lax.rem(Z + 1, 4), lax.rem(Z + 3, 4), lax.rem(Z + 2, 4)
    seen_w, seen_x = set(), set()

    def s1(j, rel):
        i = 4 * j + rel
        if j not in seen_w:
            seen_w.add(j)
            arrive(w1buf.at[j], w1_r + j)
        if rel not in seen_x:
            seen_x.add(rel)
            arrive(xbuf.at[1 - C, rel], sib_r + rel)

        @pl.loop(0, 2)
        def _(b):
            features = jnp.concatenate([xbuf[0, rel, b], xbuf[1, rel, b]], axis=1)
            weights = w1buf[j].reshape(2 * feat, WIDE)
            acc = jnp.dot(features, weights, preferred_element_type=F32)
            pbuf[i, b] = acc[:, :HEAD_DIM].astype(BF16)
            pbuf[i, 2 + b] = acc[:, HEAD_DIM:].astype(BF16)

        copy(pbuf.at[i, z2, pl.ds(0, half)], r1.at[0, i], r1_r + i, fwd, "r1")
        copy(pbuf.at[i, z2, pl.ds(half, half)], r1.at[1, i], r1_r + i, back, "r1")

    def s2(j, rel):
        i = 4 * j + rel
        arrive(r1.at[:, i], r1_r + i)
        pbuf[i, zp, pl.ds(0, half)] = (pbuf[i, zp, pl.ds(0, half)].astype(F32) + r1[0, i].astype(F32)).astype(BF16)
        copy(pbuf.at[i, zp], r2.at[0, i], r2_r + i, fwd, "r2")
        pbuf[i, zm, pl.ds(half, half)] = (
            pbuf[i, zm, pl.ds(half, half)].astype(F32) + r1[1, i].astype(F32)
        ).astype(BF16)
        copy(pbuf.at[i, zm], r2.at[1, i], r2_r + i, back, "r2")

    def s3(j, rel):
        i = 4 * j + rel
        arrive(r2.at[:, i], r2_r + i)
        whole = (pbuf[i, Z].astype(F32) + r2[0, i].astype(F32) + r2[1, i].astype(F32)).astype(BF16)
        if j < 3:
            qkv[rel, j] = whole
        if j == 2:
            query = (head_norm(qkv[rel, 0].astype(F32)) * (1.0 / HEAD_DIM) ** 0.5).astype(BF16)
            keys = head_norm(qkv[rel, 1].astype(F32)).astype(BF16)
            scores = lax.dot_general(query, keys, (((1,), (1,)), ((), ())), preferred_element_type=F32)
            weights = jnp.exp(scores)
            probs = (weights / jnp.sum(weights, axis=-1, keepdims=True)).astype(BF16)
            hbuf[rel, Z, 0] = jnp.dot(probs, whole, preferred_element_type=F32).astype(BF16)
        if j >= 3:
            hbuf[rel, Z, j - 2] = gelu(whole.astype(F32)).astype(BF16)
        if j in (3, 5):
            k = (j - 3) // 2
            mine = hbuf.at[rel, Z, pl.ds(2 * k, 2)]
            copy(mine, mine, near_r + 2 * rel + k, fwd, "near")
            copy(mine, mine, near_r + 2 * rel + k, back, "near")

    def relay(k, rel):
        arrive(hbuf.at[rel, pl.ds(0, 2), pl.ds(2 * k, 2)], near_r + 2 * rel + k)
        top = hbuf.at[rel, zm, pl.ds(2 * k, 2), pl.ds(0, half)]
        copy(top, top, far_h + rel, fwd, "far")
        low = hbuf.at[rel, zp, pl.ds(2 * k, 2), pl.ds(half, half)]
        copy(low, low, far_h + rel, back, "far")

    seen_w2, seen_h = set(), set()

    def e1(f, rel):
        if f not in seen_w2:
            seen_w2.add(f)
            arrive(w2buf.at[:, f], w2_r + f)
        if rel not in seen_h:
            seen_h.add(rel)
            arrive(hbuf.at[rel, z2], far_h + rel)

        @pl.loop(0, 2)
        def _(b):
            hidden = jnp.concatenate([hbuf[rel, 2 * h + b, k] for k in range(4) for h in range(2)], axis=1)
            both = jnp.concatenate([w2buf[0, f], w2buf[1, f]], axis=1)
            whole = jnp.dot(hidden, both, preferred_element_type=F32).astype(BF16)
            for side in range(2):
                oall[side, rel, f, b] = whole[:, side * WIDE : (side + 1) * WIDE]

        copy(oall.at[1 - C, rel, f], osib.at[rel, f], e_r + rel * PARTS + f, sib, "cores")

    ry_r = sems("r", 3 * PARTS)
    xr_r = sems("r", 2 * PARTS)
    xr_s = sems("s", 2 * PARTS)

    def final_copy(b, f):
        return pltpu.make_async_remote_copy(
            src_ref=xsend.at[f, b], dst_ref=xrecv.at[f, L], send_sem=send_sem.at[xr_s + 2 * f + b],
            recv_sem=recv_sem.at[xr_r + 2 * f + L], device_id={"H": C, "L": b, "C": H}, device_id_type=MESH,
        )

    def e2(f, rel):
        arrive(osib.at[rel, f], e_r + rel * PARTS + f)
        ry = ry_r + 3 * f
        for b in range(2):
            total = oall[C, rel, f, b].astype(F32) + osib[rel, f, b].astype(F32)
            if rel == 1 and b == 0:
                arrive(ry1.at[f, 0], ry)
                total = total + ry1[f, 0].astype(F32)
            if rel == 3 and b == 1:
                arrive(ry1.at[f, 1], ry + 1)
                total = total + ry1[f, 1].astype(F32)
            if rel == 0:
                if b == 0:
                    arrive(ry2.at[f], ry + 2)
                xsend[f, b] = (total + ry2[f, 0, b].astype(F32) + ry2[f, 1, b].astype(F32)).astype(BF16)
                mine = jnp.logical_and(C == H, L == b)

                @pl.when(mine)
                def _():
                    xrecv[f, b] = xsend[f, b]

                @pl.when(jnp.logical_not(mine))
                def _():
                    final_copy(b, f).start()
            else:
                oall[C, rel, f, b] = total.astype(BF16)
        if rel == 2:
            copy(oall.at[C, 2, f, 0], ry1.at[f, 0], ry, up, "ry1")
            copy(oall.at[C, 2, f, 1], ry1.at[f, 1], ry + 1, down, "ry1")
        if rel == 1:
            copy(oall.at[C, 1, f], ry2.at[f, 0], ry + 2, up, "ry2")
        if rel == 3:
            copy(oall.at[C, 3, f], ry2.at[f, 1], ry + 2, down, "ry2")

    stages = {
        "y1": lambda a, rel: relay_y(early),
        "y2": lambda a, rel: relay_y(1 - early),
        "y3": lambda a, rel: far_y(),
        "s1": s1, "s2": s2, "s3": s3, "s4": relay, "e1": e1, "e2": e2,
    }
    for stage, a, rel in ORDER:
        stages[stage](a, rel)

    for f in range(PARTS):
        for b in range(2):

            @pl.when(jnp.logical_not(jnp.logical_and(C == H, L == b)))
            def _():
                arrive(xrecv.at[f, b], xr_r + 2 * f + b)

        columns = pl.ds(f * WIDE, WIDE)
        out[:, columns] = (
            tok[:, columns].astype(F32) + xrecv[f, 0].astype(F32) + xrecv[f, 1].astype(F32)
        ).astype(BF16)

    for n, r in enumerate(readers):
        unless(straight, r == (0, 0, 0), lambda: stat_copy(n).wait_send())
    whole = {
        "w1": w1buf, "w2": w2buf, "y": xbuf.at[0, pl.ds(0, 3)], "core": xbuf.at[0], "r1": r1, "r2": r2,
        "near": hbuf.at[pl.ds(0, 2)], "far": hbuf.at[0], "cores": osib, "ry1": ry1, "ry2": ry2,
    }
    for kind, (sem, total) in pending.items():
        ref = whole[kind]
        assert size(ref) == total, kind
        pltpu.make_async_remote_copy(
            src_ref=ref, dst_ref=ref, send_sem=send_sem.at[sem], recv_sem=recv_sem.at[0],
            device_id=sib, device_id_type=MESH,
        ).wait_send()
    for b in range(2):

        @pl.when(jnp.logical_not(jnp.logical_and(C == H, L == b)))
        def _():
            for n in range(2):
                token_copy(b, n).wait_send()

        @pl.when(jnp.logical_not(jnp.logical_and(C == H, L == b)))
        def _():
            for f in range(PARTS):
                final_copy(b, f).wait_send()

    assert count["s"] <= N_SEND and count["r"] <= N_RECV, count


def local(tokens, norm_gain, w_qkv, w_up, w_attn_out, w_down):
    rows, feat = tokens.shape
    width = feat * lax.axis_size("H") * lax.axis_size("Z")
    n_items = 4 * CHUNKS
    half = rows // 2
    vmem = pltpu.VMEM
    out_part = (PARTS, 2, rows, WIDE)
    scratch = [
        vmem((8, rows), F32),
        vmem((2, 2, 4, 8, rows), F32),
        vmem((2, rows, feat), BF16),
        vmem((2, 4, 2, rows, feat), BF16),
        vmem((CHUNKS, 2, feat, WIDE), BF16),
        vmem((2, PARTS, w_attn_out.shape[0] + w_down.shape[0], WIDE), BF16),
        vmem((n_items, 4, rows, HEAD_DIM), BF16),
        vmem((2, n_items, half, HEAD_DIM), BF16),
        vmem((2, n_items, rows, HEAD_DIM), BF16),
        vmem((4, 3, rows, HEAD_DIM), BF16),
        vmem((4, 4, 4, rows, HEAD_DIM), BF16),
        vmem((2, 4, *out_part), BF16),
        vmem((4, *out_part), BF16),
        vmem((PARTS, 2, rows, WIDE), BF16),
        vmem((PARTS, 2, 2, rows, WIDE), BF16),
        vmem(out_part, BF16),
        vmem(out_part, BF16),
        pltpu.SemaphoreType.DMA((N_SEND,)),
        pltpu.SemaphoreType.DMA((N_RECV,)),
    ]
    in_vmem = pl.BlockSpec(memory_space=pltpu.VMEM)
    anywhere = pl.BlockSpec(memory_space=pl.ANY)
    return pl.pallas_call(
        functools.partial(kernel, width),
        out_shape=jax.ShapeDtypeStruct((rows, feat), BF16),
        in_specs=[in_vmem] * 2 + [anywhere] * 4,
        out_specs=in_vmem,
        scratch_shapes=scratch,
        compiler_params=pltpu.CompilerParams(
            collective_id=0, has_side_effects=True, vmem_limit_bytes=60 * 1024 * 1024
        ),
        name="layer",
    )(tokens, norm_gain, w_qkv.transpose(1, 0, 2), w_up, w_attn_out, w_down)


def solution(mesh):
    torus = Mesh(mesh.devices.reshape(2, 4, 2, 2, 4), ("L", "Y", "C", "H", "Z"))
    in_specs = (P(DP, MP), P(MP), P(MP, None, DP), P(MP, DP), P(DP, MP), P(DP, MP))
    return jax.shard_map(local, mesh=torus, in_specs=in_specs, out_specs=P(DP, MP), check_vma=False)
```

```python
import functools
import math

import jax
import jax.numpy as jnp
from jax import lax
from jax.experimental import pallas as pl
from jax.experimental.pallas import tpu as pltpu
from jax.sharding import Mesh
from jax.sharding import PartitionSpec as P

HEAD_DIM = 128
PATCHES = 256
EPS = 1e-06
MESH = pl.DeviceIdType.MESH
F32 = jnp.float32
BF16 = jnp.bfloat16
DP = ("L", "Y", "C")
MP = ("H", "Z")

CHUNKS = 6
WIDE = 2 * HEAD_DIM
PARTS = 3
ORDER = (
    ("y1", 0, 0), ("s1", 0, 0), ("y2", 0, 0), ("s2", 0, 0), ("s1", 1, 0), ("s1", 0, 1), ("s1", 1, 1), ("s1", 0, 3),
    ("s2", 1, 0), ("s1", 1, 3), ("s2", 0, 1), ("s2", 0, 3), ("y3", 0, 0), ("s1", 2, 2), ("s1", 1, 2), ("s2", 1, 1),
    ("s2", 1, 3), ("s1", 0, 2), ("s1", 2, 1), ("s1", 2, 3), ("s2", 1, 2), ("s2", 2, 2), ("s1", 3, 2), ("s2", 0, 2),
    ("s2", 2, 1), ("s2", 3, 2), ("s1", 3, 1), ("s3", 0, 1), ("s3", 0, 2), ("s3", 1, 2), ("s3", 0, 3), ("s1", 3, 3),
    ("s2", 2, 3), ("s3", 1, 3), ("s3", 2, 2), ("s1", 4, 3), ("s1", 3, 0), ("s2", 3, 1), ("s3", 1, 1), ("s1", 4, 2),
    ("s1", 4, 1), ("s2", 4, 3), ("s3", 3, 2), ("s1", 5, 2), ("s1", 5, 3), ("s2", 4, 1), ("s3", 2, 1), ("s1", 5, 1),
    ("s2", 4, 2), ("s3", 2, 3), ("s2", 5, 2), ("s2", 5, 3), ("s4", 0, 2), ("s3", 4, 2), ("s2", 3, 3), ("s2", 5, 1),
    ("s3", 5, 2), ("s3", 3, 3), ("s3", 3, 1), ("s3", 4, 1), ("s3", 4, 3), ("s4", 1, 2), ("s3", 5, 1), ("s3", 5, 3),
    ("s1", 4, 0), ("s3", 0, 0), ("s1", 2, 0), ("e1", 0, 2), ("s4", 0, 1), ("s4", 1, 1), ("s4", 1, 3), ("e1", 1, 2),
    ("s1", 5, 0), ("s3", 1, 0), ("e2", 0, 2), ("e1", 2, 2), ("s4", 0, 3), ("s2", 2, 0), ("e2", 1, 2), ("s2", 3, 0),
    ("e1", 1, 1), ("e1", 0, 1), ("s2", 4, 0), ("e2", 2, 2), ("e1", 0, 3), ("s2", 5, 0), ("s3", 2, 0), ("s3", 3, 0),
    ("e2", 0, 1), ("e2", 0, 3), ("e2", 1, 1), ("s3", 4, 0), ("s3", 5, 0), ("e1", 1, 3), ("e2", 1, 3), ("e1", 2, 1),
    ("s4", 0, 0), ("e1", 2, 3), ("s4", 1, 0), ("e2", 2, 1), ("e2", 2, 3), ("e1", 0, 0), ("e1", 1, 0), ("e2", 0, 0),
    ("e1", 2, 0), ("e2", 1, 0), ("e2", 2, 0),
)
N_SEND = 37
N_RECV = 129


def gelu(u):
    return 0.5 * u * (1.0 + jnp.tanh(0.7978845608028654 * (u + 0.044715 * (u * u * u))))


def head_norm(values):
    mean = jnp.mean(values, axis=-1, keepdims=True)
    centered = values - mean
    spread = jnp.mean(centered * centered, axis=-1, keepdims=True)
    return centered * lax.rsqrt(spread + EPS)


def kernel(
    width,
    tok, gain, w_qkv, w_up, w_attn, w_down,
    out,
    stats, statbuf, xraw, xbuf, w1buf, w2buf, pbuf, r1, r2, qkv, hbuf, oall, osib, ry1, ry2, xsend, xrecv,
    send_sem, recv_sem,
):
    L, Y, C, H, Z = (lax.axis_index(a) for a in ("L", "Y", "C", "H", "Z"))
    rows, feat = tok.shape
    half = rows // 2
    near = ({"L": 1 - L, "H": C}, {"L": 1 - L, "H": 1 - C})
    up, down = {"Y": lax.rem(Y + 1, 4)}, {"Y": lax.rem(Y + 3, 4)}
    fwd, back = {"Z": lax.rem(Z + 1, 4)}, {"Z": lax.rem(Z + 3, 4)}
    sib = {"C": 1 - C}
    swapped = (C != H).astype(jnp.int32)
    straight = C == H

    count = {"s": 0, "r": 0}
    pending = {}

    def sems(kind, n=1):
        first = count[kind]
        count[kind] += n
        return first

    def size(ref):
        return math.prod(ref.shape) * 2

    def copy(src, dst, recv, dev, kind):
        if kind not in pending:
            pending[kind] = [sems("s"), 0]
        pending[kind][1] += size(src)
        pltpu.make_async_remote_copy(
            src_ref=src, dst_ref=dst, send_sem=send_sem.at[pending[kind][0]], recv_sem=recv_sem.at[recv],
            device_id=dev, device_id_type=MESH,
        ).start()

    def arrive(dst, recv):
        pltpu.make_async_remote_copy(
            src_ref=dst, dst_ref=dst, send_sem=send_sem.at[0], recv_sem=recv_sem.at[recv],
            device_id=sib, device_id_type=MESH,
        ).wait_recv()

    barrier = pltpu.get_barrier_semaphore()
    for dev in (*near, up, down, fwd, back, sib):
        pl.semaphore_signal(barrier, inc=1, device_id=dev, device_id_type=MESH)

    readers = [(dl, dz, dc) for dl in range(2) for dz in range(4) for dc in range(2)]

    def reader(dl, dz, dc):
        return {"H": C, "L": lax.rem(L + dl, 2), "Z": lax.rem(Z + dz, 4), "C": lax.rem(C + dc, 2)}

    def unless(condition, skip, f):
        if skip:
            pl.when(jnp.logical_not(condition))(f)
        else:
            f()

    for dh, dl, dz in [(dh, dl, dz) for dh in range(2) for dl in range(2) for dz in range(4)]:

        def greet():
            source = {"C": H, "H": lax.rem(H + dh, 2), "L": lax.rem(L + dl, 2), "Z": lax.rem(Z + dz, 4)}
            pl.semaphore_signal(barrier, inc=1, device_id=source, device_id_type=MESH)

        unless(straight, dh + dl + dz == 0, greet)

    w1_r = sems("r", CHUNKS)
    w2_r = sems("r", PARTS)

    def send_w1(j, dev):
        block = w_qkv.at[j] if j < 3 else w_up.at[:, pl.ds((j - 3) * WIDE, WIDE)]
        copy(block, w1buf.at[j, H], w1_r + j, dev, "w1")

    def send_w2(f, dev):
        top, columns = w_attn.shape[0], pl.ds(f * WIDE, WIDE)
        copy(w_attn.at[:, columns], w2buf.at[H, f, pl.ds(0, top)], w2_r + f, dev, "w2")
        copy(w_down.at[:, columns], w2buf.at[H, f, pl.ds(top, w_down.shape[0])], w2_r + f, dev, "w2")

    tokens_f = tok[...].astype(F32)
    lane = lax.broadcasted_iota(jnp.int32, (rows, 128), 1)
    total = jnp.sum(tokens_f, axis=1, keepdims=True)
    squares = jnp.sum(tokens_f * tokens_f, axis=1, keepdims=True)
    stats[...] = jnp.transpose(jnp.where(lane == 0, total, jnp.where(lane == 1, squares, 0.0)))[0:8]
    for k in range(feat // rows):
        stats[pl.ds(2 + k, 1)] = gain[pl.ds(k * rows, rows)][None, :]

    pl.semaphore_wait(barrier, 23 - straight.astype(jnp.int32))

    stat_r = sems("r", 16)
    stat_s = sems("s", 16)

    def stat_copy(n):
        dl, dz, dc = readers[n]
        return pltpu.make_async_remote_copy(
            src_ref=stats, dst_ref=statbuf.at[H, dl, dz], send_sem=send_sem.at[stat_s + n],
            recv_sem=recv_sem.at[stat_r + 8 * H + 4 * dl + dz], device_id=reader(dl, dz, dc), device_id_type=MESH,
        )

    for n, r in enumerate(readers):
        unless(straight, r == (0, 0, 0), lambda: stat_copy(n).start())

    x_r = sems("r", 4)
    x_s = sems("s", 4)

    first, second = pl.ds(0, half), pl.ds(half, half)
    halves = (first, second)

    def token_copy(b, n):
        return pltpu.make_async_remote_copy(
            src_ref=tok.at[halves[n]], dst_ref=xraw.at[L, halves[n]], send_sem=send_sem.at[x_s + 2 * b + n],
            recv_sem=recv_sem.at[x_r + 2 * L + n], device_id={"H": C, "L": b, "C": H}, device_id_type=MESH,
        )

    for b in (1 - L, L):
        mine = jnp.logical_and(straight, L == b)

        @pl.when(jnp.logical_not(mine))
        def _():
            for n in range(2):
                token_copy(b, n).start()

    send_w1(0, near[0])

    @pl.when(straight)
    def _():
        xraw[L] = tok[...]
        statbuf[H, 0, 0] = stats[...]

    yp_r, ym_r, far_r, sib_r = sems("r", 4), sems("r", 4), sems("r"), sems("r", 4)

    def to_sib(rel, b):
        copy(xbuf.at[C, rel, b], xbuf.at[C, rel, b], sib_r + rel, sib, "core")

    early = lax.rem(L + swapped, 2)

    def start_y(b):
        mine = jnp.logical_and(straight, L == b)
        dl = lax.rem(L + b, 2)

        @pl.when(jnp.logical_not(mine))
        def _():
            arrive(statbuf.at[H, dl, 0], stat_r + 8 * H + 4 * dl)

        arrive(statbuf.at[1 - H, dl, 0], stat_r + 8 * (1 - H) + 4 * dl)
        for src in range(2):
            for dz in range(1, 4):
                arrive(statbuf.at[src, dl, dz], stat_r + 8 * src + 4 * dl + dz)
        summed = statbuf[0, dl, 0]
        for src, dz in [(0, 1), (0, 2), (0, 3), (1, 0), (1, 1), (1, 2), (1, 3)]:
            summed = summed + statbuf[src, dl, dz]
        column = jnp.transpose(jnp.concatenate([summed] * 16, axis=0))
        mean = column[:, 0:1] / width
        spread = column[:, 1:2] / width - mean * mean
        scale = lax.rsqrt(spread + EPS)
        gains = jnp.concatenate([statbuf[C, dl, 0, pl.ds(2 + k, 1)] for k in range(feat // rows)], axis=1)

        for n, part in enumerate(halves):

            @pl.when(jnp.logical_not(mine))
            def _():
                arrive(xraw.at[b, part], x_r + 2 * b + n)

            at = slice(n * half, (n + 1) * half)
            xbuf[C, 0, b, part] = ((xraw[b, part].astype(F32) - mean[at]) * scale[at] * gains).astype(BF16)
            copy(xbuf.at[C, 0, b, part], xbuf.at[C, 3, b, part], yp_r + 2 * b + n, up, "y")
            copy(xbuf.at[C, 0, b, part], xbuf.at[C, 1, b, part], ym_r + 2 * b + n, down, "y")
        to_sib(0, b)

    def relay_y(b):
        arrive(xbuf.at[C, 3, b, first], yp_r + 2 * b)
        copy(xbuf.at[C, 3, b, first], xbuf.at[C, 2, b, first], far_r, up, "y")
        arrive(xbuf.at[C, 1, b, first], ym_r + 2 * b)
        arrive(xbuf.at[C, 1, b, second], ym_r + 2 * b + 1)
        copy(xbuf.at[C, 1, b, second], xbuf.at[C, 2, b, second], far_r, down, "y")
        to_sib(1, b)
        arrive(xbuf.at[C, 3, b, second], yp_r + 2 * b + 1)
        to_sib(3, b)

    def far_y():
        arrive(xbuf.at[C, 2], far_r)
        for b in range(2):
            to_sib(2, b)

    start_y(early)
    start_y(1 - early)
    send_w1(0, near[1])
    for j in range(1, CHUNKS):
        for dev in near:
            send_w1(j, dev)
    for f in range(PARTS):
        for dev in near:
            send_w2(f, dev)

    n_items = 4 * CHUNKS
    r1_r, r2_r = sems("r", n_items), sems("r", n_items)
    near_r, far_h = sems("r", 8), sems("r", 4)
    e_r = sems("r", 4 * PARTS)
    zp, zm, z2 = lax.rem(Z + 1, 4), lax.rem(Z + 3, 4), lax.rem(Z + 2, 4)
    seen_w, seen_x = set(), set()

    def s1(j, rel):
        i = 4 * j + rel
        if j not in seen_w:
            seen_w.add(j)
            arrive(w1buf.at[j], w1_r + j)
        if rel not in seen_x:
            seen_x.add(rel)
            arrive(xbuf.at[1 - C, rel], sib_r + rel)

        @pl.loop(0, 2)
        def _(b):
            features = jnp.concatenate([xbuf[0, rel, b], xbuf[1, rel, b]], axis=1)
            weights = w1buf[j].reshape(2 * feat, WIDE)
            acc = jnp.dot(features, weights, preferred_element_type=F32)
            pbuf[i, b] = acc[:, :HEAD_DIM].astype(BF16)
            pbuf[i, 2 + b] = acc[:, HEAD_DIM:].astype(BF16)

        copy(pbuf.at[i, z2, pl.ds(0, half)], r1.at[0, i], r1_r + i, fwd, "r1")
        copy(pbuf.at[i, z2, pl.ds(half, half)], r1.at[1, i], r1_r + i, back, "r1")

    def s2(j, rel):
        i = 4 * j + rel
        arrive(r1.at[:, i], r1_r + i)
        pbuf[i, zp, pl.ds(0, half)] = (pbuf[i, zp, pl.ds(0, half)].astype(F32) + r1[0, i].astype(F32)).astype(BF16)
        copy(pbuf.at[i, zp], r2.at[0, i], r2_r + i, fwd, "r2")
        pbuf[i, zm, pl.ds(half, half)] = (
            pbuf[i, zm, pl.ds(half, half)].astype(F32) + r1[1, i].astype(F32)
        ).astype(BF16)
        copy(pbuf.at[i, zm], r2.at[1, i], r2_r + i, back, "r2")

    def s3(j, rel):
        i = 4 * j + rel
        arrive(r2.at[:, i], r2_r + i)
        whole = (pbuf[i, Z].astype(F32) + r2[0, i].astype(F32) + r2[1, i].astype(F32)).astype(BF16)
        if j < 3:
            qkv[rel, j] = whole
        if j == 2:
            query = (head_norm(qkv[rel, 0].astype(F32)) * (1.0 / HEAD_DIM) ** 0.5).astype(BF16)
            keys = head_norm(qkv[rel, 1].astype(F32)).astype(BF16)
            scores = lax.dot_general(query, keys, (((1,), (1,)), ((), ())), preferred_element_type=F32)
            weights = jnp.exp(scores)
            probs = (weights / jnp.sum(weights, axis=-1, keepdims=True)).astype(BF16)
            hbuf[rel, Z, 0] = jnp.dot(probs, whole, preferred_element_type=F32).astype(BF16)
        if j >= 3:
            hbuf[rel, Z, j - 2] = gelu(whole.astype(F32)).astype(BF16)
        if j in (3, 5):
            k = (j - 3) // 2
            mine = hbuf.at[rel, Z, pl.ds(2 * k, 2)]
            copy(mine, mine, near_r + 2 * rel + k, fwd, "near")
            copy(mine, mine, near_r + 2 * rel + k, back, "near")

    def relay(k, rel):
        arrive(hbuf.at[rel, pl.ds(0, 2), pl.ds(2 * k, 2)], near_r + 2 * rel + k)
        top = hbuf.at[rel, zm, pl.ds(2 * k, 2), pl.ds(0, half)]
        copy(top, top, far_h + rel, fwd, "far")
        low = hbuf.at[rel, zp, pl.ds(2 * k, 2), pl.ds(half, half)]
        copy(low, low, far_h + rel, back, "far")

    seen_w2, seen_h = set(), set()

    def e1(f, rel):
        if f not in seen_w2:
            seen_w2.add(f)
            arrive(w2buf.at[:, f], w2_r + f)
        if rel not in seen_h:
            seen_h.add(rel)
            arrive(hbuf.at[rel, z2], far_h + rel)

        @pl.loop(0, 2)
        def _(b):
            hidden = jnp.concatenate([hbuf[rel, 2 * h + b, k] for k in range(4) for h in range(2)], axis=1)
            both = jnp.concatenate([w2buf[0, f], w2buf[1, f]], axis=1)
            whole = jnp.dot(hidden, both, preferred_element_type=F32).astype(BF16)
            for side in range(2):
                oall[side, rel, f, b] = whole[:, side * WIDE : (side + 1) * WIDE]

        copy(oall.at[1 - C, rel, f], osib.at[rel, f], e_r + rel * PARTS + f, sib, "cores")

    ry_r = sems("r", 3 * PARTS)
    xr_r = sems("r", 2 * PARTS)
    xr_s = sems("s", 2 * PARTS)

    def final_copy(b, f):
        return pltpu.make_async_remote_copy(
            src_ref=xsend.at[f, b], dst_ref=xrecv.at[f, L], send_sem=send_sem.at[xr_s + 2 * f + b],
            recv_sem=recv_sem.at[xr_r + 2 * f + L], device_id={"H": C, "L": b, "C": H}, device_id_type=MESH,
        )

    def e2(f, rel):
        arrive(osib.at[rel, f], e_r + rel * PARTS + f)
        ry = ry_r + 3 * f
        for b in range(2):
            total = oall[C, rel, f, b].astype(F32) + osib[rel, f, b].astype(F32)
            if rel == 1 and b == 0:
                arrive(ry1.at[f, 0], ry)
                total = total + ry1[f, 0].astype(F32)
            if rel == 3 and b == 1:
                arrive(ry1.at[f, 1], ry + 1)
                total = total + ry1[f, 1].astype(F32)
            if rel == 0:
                if b == 0:
                    arrive(ry2.at[f], ry + 2)
                xsend[f, b] = (total + ry2[f, 0, b].astype(F32) + ry2[f, 1, b].astype(F32)).astype(BF16)
                mine = jnp.logical_and(C == H, L == b)

                @pl.when(mine)
                def _():
                    xrecv[f, b] = xsend[f, b]

                @pl.when(jnp.logical_not(mine))
                def _():
                    final_copy(b, f).start()
            else:
                oall[C, rel, f, b] = total.astype(BF16)
        if rel == 2:
            copy(oall.at[C, 2, f, 0], ry1.at[f, 0], ry, up, "ry1")
            copy(oall.at[C, 2, f, 1], ry1.at[f, 1], ry + 1, down, "ry1")
        if rel == 1:
            copy(oall.at[C, 1, f], ry2.at[f, 0], ry + 2, up, "ry2")
        if rel == 3:
            copy(oall.at[C, 3, f], ry2.at[f, 1], ry + 2, down, "ry2")

    stages = {
        "y1": lambda a, rel: relay_y(early),
        "y2": lambda a, rel: relay_y(1 - early),
        "y3": lambda a, rel: far_y(),
        "s1": s1, "s2": s2, "s3": s3, "s4": relay, "e1": e1, "e2": e2,
    }
    for stage, a, rel in ORDER:
        stages[stage](a, rel)

    for f in range(PARTS):
        for b in range(2):

            @pl.when(jnp.logical_not(jnp.logical_and(C == H, L == b)))
            def _():
                arrive(xrecv.at[f, b], xr_r + 2 * f + b)

        columns = pl.ds(f * WIDE, WIDE)
        out[:, columns] = (
            tok[:, columns].astype(F32) + xrecv[f, 0].astype(F32) + xrecv[f, 1].astype(F32)
        ).astype(BF16)

    for n, r in enumerate(readers):
        unless(straight, r == (0, 0, 0), lambda: stat_copy(n).wait_send())
    whole = {
        "w1": w1buf, "w2": w2buf, "y": xbuf.at[0, pl.ds(0, 3)], "core": xbuf.at[0], "r1": r1, "r2": r2,
        "near": hbuf.at[pl.ds(0, 2)], "far": hbuf.at[0], "cores": osib, "ry1": ry1, "ry2": ry2,
    }
    for kind, (sem, total) in pending.items():
        ref = whole[kind]
        assert size(ref) == total, kind
        pltpu.make_async_remote_copy(
            src_ref=ref, dst_ref=ref, send_sem=send_sem.at[sem], recv_sem=recv_sem.at[0],
            device_id=sib, device_id_type=MESH,
        ).wait_send()
    for b in range(2):

        @pl.when(jnp.logical_not(jnp.logical_and(C == H, L == b)))
        def _():
            for n in range(2):
                token_copy(b, n).wait_send()

        @pl.when(jnp.logical_not(jnp.logical_and(C == H, L == b)))
        def _():
            for f in range(PARTS):
                final_copy(b, f).wait_send()

    assert count["s"] <= N_SEND and count["r"] <= N_RECV, count


def local(tokens, norm_gain, w_qkv, w_up, w_attn_out, w_down):
    rows, feat = tokens.shape
    width = feat * lax.axis_size("H") * lax.axis_size("Z")
    n_items = 4 * CHUNKS
    half = rows // 2
    vmem = pltpu.VMEM
    out_part = (PARTS, 2, rows, WIDE)
    scratch = [
        vmem((8, rows), F32),
        vmem((2, 2, 4, 8, rows), F32),
        vmem((2, rows, feat), BF16),
        vmem((2, 4, 2, rows, feat), BF16),
        vmem((CHUNKS, 2, feat, WIDE), BF16),
        vmem((2, PARTS, w_attn_out.shape[0] + w_down.shape[0], WIDE), BF16),
        vmem((n_items, 4, rows, HEAD_DIM), BF16),
        vmem((2, n_items, half, HEAD_DIM), BF16),
        vmem((2, n_items, rows, HEAD_DIM), BF16),
        vmem((4, 3, rows, HEAD_DIM), BF16),
        vmem((4, 4, 4, rows, HEAD_DIM), BF16),
        vmem((2, 4, *out_part), BF16),
        vmem((4, *out_part), BF16),
        vmem((PARTS, 2, rows, WIDE), BF16),
        vmem((PARTS, 2, 2, rows, WIDE), BF16),
        vmem(out_part, BF16),
        vmem(out_part, BF16),
        pltpu.SemaphoreType.DMA((N_SEND,)),
        pltpu.SemaphoreType.DMA((N_RECV,)),
    ]
    in_vmem = pl.BlockSpec(memory_space=pltpu.VMEM)
    anywhere = pl.BlockSpec(memory_space=pl.ANY)
    return pl.pallas_call(
        functools.partial(kernel, width),
        out_shape=jax.ShapeDtypeStruct((rows, feat), BF16),
        in_specs=[in_vmem] * 2 + [anywhere] * 4,
        out_specs=in_vmem,
        scratch_shapes=scratch,
        compiler_params=pltpu.CompilerParams(
            collective_id=0, has_side_effects=True, vmem_limit_bytes=60 * 1024 * 1024
        ),
        name="layer",
    )(tokens, norm_gain, w_qkv.transpose(1, 0, 2), w_up, w_attn_out, w_down)


def solution(mesh):
    torus = Mesh(mesh.devices.reshape(2, 4, 2, 2, 4), ("L", "Y", "C", "H", "Z"))
    in_specs = (P(DP, MP), P(MP), P(MP, None, DP), P(MP, DP), P(DP, MP), P(DP, MP))
    return jax.shard_map(local, mesh=torus, in_specs=in_specs, out_specs=P(DP, MP), check_vma=False)
```

```python
import functools
import math

import jax
import jax.numpy as jnp
from jax import lax
from jax.experimental import pallas as pl
from jax.experimental.pallas import tpu as pltpu
from jax.sharding import Mesh
from jax.sharding import PartitionSpec as P

HEAD_DIM = 128
PATCHES = 256
EPS = 1e-06
MESH = pl.DeviceIdType.MESH
F32 = jnp.float32
BF16 = jnp.bfloat16
DP = ("L", "Y", "C")
MP = ("H", "Z")

CHUNKS = 6
WIDE = 2 * HEAD_DIM
PARTS = 3
ORDER = (
    ("y1", 0, 0), ("s1", 0, 0), ("y2", 0, 0), ("s2", 0, 0), ("s1", 1, 0), ("s1", 0, 1), ("s1", 1, 3), ("s1", 1, 1),
    ("s2", 1, 0), ("s1", 0, 3), ("s2", 0, 1), ("s2", 1, 3), ("s1", 2, 3), ("s2", 1, 1), ("s2", 0, 3), ("y3", 0, 0),
    ("s1", 2, 2), ("s2", 2, 3), ("s1", 1, 2), ("s1", 0, 2), ("s1", 2, 1), ("s2", 2, 2), ("s3", 0, 1), ("s1", 3, 3),
    ("s1", 3, 2), ("s3", 1, 1), ("s1", 3, 1), ("s2", 0, 2), ("s2", 2, 1), ("s2", 1, 2), ("s2", 3, 1), ("s2", 3, 3),
    ("s1", 4, 1), ("s3", 0, 3), ("s1", 4, 2), ("s3", 0, 2), ("s1", 4, 3), ("s3", 1, 2), ("s3", 2, 1), ("s1", 2, 0),
    ("s3", 3, 1), ("s2", 3, 2), ("s3", 2, 2), ("s2", 4, 3), ("s1", 5, 1), ("s1", 5, 2), ("s2", 4, 2), ("s3", 3, 2),
    ("s3", 1, 3), ("s3", 2, 3), ("s2", 5, 2), ("s2", 5, 1), ("s3", 3, 3), ("s4", 0, 2), ("s2", 4, 1), ("s1", 5, 3),
    ("s3", 4, 2), ("s3", 5, 2), ("s1", 4, 0), ("s1", 5, 0), ("s1", 3, 0), ("s2", 5, 3), ("s3", 4, 1), ("s3", 5, 1),
    ("s4", 1, 2), ("s3", 4, 3), ("s3", 5, 3), ("s4", 1, 1), ("e1", 1, 2), ("s4", 0, 1), ("s3", 0, 0), ("s4", 0, 3),
    ("s4", 1, 3), ("e2", 1, 2), ("e1", 0, 2), ("s2", 2, 0), ("e1", 2, 2), ("s2", 3, 0), ("s2", 4, 0), ("s2", 5, 0),
    ("s3", 1, 0), ("e2", 0, 2), ("e1", 0, 1), ("e1", 1, 1), ("e2", 2, 2), ("e1", 0, 3), ("e1", 2, 1), ("s3", 2, 0),
    ("s3", 3, 0), ("e2", 1, 1), ("e2", 0, 1), ("e2", 0, 3), ("s3", 4, 0), ("s3", 5, 0), ("e1", 1, 3), ("e1", 2, 3),
    ("e2", 1, 3), ("s4", 0, 0), ("e2", 2, 1), ("s4", 1, 0), ("e2", 2, 3), ("e1", 1, 0), ("e2", 1, 0), ("e1", 0, 0),
    ("e2", 0, 0), ("e1", 2, 0), ("e2", 2, 0),
)
N_SEND = 37
N_RECV = 129


def gelu(u):
    return 0.5 * u * (1.0 + jnp.tanh(0.7978845608028654 * (u + 0.044715 * (u * u * u))))


def head_norm(values):
    mean = jnp.mean(values, axis=-1, keepdims=True)
    centered = values - mean
    spread = jnp.mean(centered * centered, axis=-1, keepdims=True)
    return centered * lax.rsqrt(spread + EPS)


def kernel(
    width,
    tok, gain, w_qkv, w_up, w_attn, w_down,
    out,
    stats, statbuf, xraw, xbuf, w1buf, w2buf, pbuf, r1, r2, qkv, hbuf, oall, osib, ry1, ry2, xsend, xrecv,
    send_sem, recv_sem,
):
    L, Y, C, H, Z = (lax.axis_index(a) for a in ("L", "Y", "C", "H", "Z"))
    rows, feat = tok.shape
    half = rows // 2
    near = ({"L": 1 - L, "H": C}, {"L": 1 - L, "H": 1 - C})
    up, down = {"Y": lax.rem(Y + 1, 4)}, {"Y": lax.rem(Y + 3, 4)}
    fwd, back = {"Z": lax.rem(Z + 1, 4)}, {"Z": lax.rem(Z + 3, 4)}
    sib = {"C": 1 - C}
    swapped = (C != H).astype(jnp.int32)
    straight = C == H

    count = {"s": 0, "r": 0}
    pending = {}

    def sems(kind, n=1):
        first = count[kind]
        count[kind] += n
        return first

    def size(ref):
        return math.prod(ref.shape) * 2

    def copy(src, dst, recv, dev, kind):
        if kind not in pending:
            pending[kind] = [sems("s"), 0]
        pending[kind][1] += size(src)
        pltpu.make_async_remote_copy(
            src_ref=src, dst_ref=dst, send_sem=send_sem.at[pending[kind][0]], recv_sem=recv_sem.at[recv],
            device_id=dev, device_id_type=MESH,
        ).start()

    def arrive(dst, recv):
        pltpu.make_async_remote_copy(
            src_ref=dst, dst_ref=dst, send_sem=send_sem.at[0], recv_sem=recv_sem.at[recv],
            device_id=sib, device_id_type=MESH,
        ).wait_recv()

    barrier = pltpu.get_barrier_semaphore()
    for dev in (*near, up, down, fwd, back, sib):
        pl.semaphore_signal(barrier, inc=1, device_id=dev, device_id_type=MESH)

    readers = [(dl, dz, dc) for dl in range(2) for dz in range(4) for dc in range(2)]

    def reader(dl, dz, dc):
        return {"H": C, "L": lax.rem(L + dl, 2), "Z": lax.rem(Z + dz, 4), "C": lax.rem(C + dc, 2)}

    def unless(condition, skip, f):
        if skip:
            pl.when(jnp.logical_not(condition))(f)
        else:
            f()

    for dh, dl, dz in [(dh, dl, dz) for dh in range(2) for dl in range(2) for dz in range(4)]:

        def greet():
            source = {"C": H, "H": lax.rem(H + dh, 2), "L": lax.rem(L + dl, 2), "Z": lax.rem(Z + dz, 4)}
            pl.semaphore_signal(barrier, inc=1, device_id=source, device_id_type=MESH)

        unless(straight, dh + dl + dz == 0, greet)

    w1_r = sems("r", CHUNKS)
    w2_r = sems("r", PARTS)

    def send_w1(j, dev):
        block = w_qkv.at[j] if j < 3 else w_up.at[:, pl.ds((j - 3) * WIDE, WIDE)]
        copy(block, w1buf.at[j, H], w1_r + j, dev, "w1")

    def send_w2(f, dev):
        top, columns = w_attn.shape[0], pl.ds(f * WIDE, WIDE)
        copy(w_attn.at[:, columns], w2buf.at[H, f, pl.ds(0, top)], w2_r + f, dev, "w2")
        copy(w_down.at[:, columns], w2buf.at[H, f, pl.ds(top, w_down.shape[0])], w2_r + f, dev, "w2")

    tokens_f = tok[...].astype(F32)
    lane = lax.broadcasted_iota(jnp.int32, (rows, 128), 1)
    total = jnp.sum(tokens_f, axis=1, keepdims=True)
    squares = jnp.sum(tokens_f * tokens_f, axis=1, keepdims=True)
    stats[...] = jnp.transpose(jnp.where(lane == 0, total, jnp.where(lane == 1, squares, 0.0)))[0:8]
    for k in range(feat // rows):
        stats[pl.ds(2 + k, 1)] = gain[pl.ds(k * rows, rows)][None, :]

    pl.semaphore_wait(barrier, 23 - straight.astype(jnp.int32))

    stat_r = sems("r", 16)
    stat_s = sems("s", 16)

    def stat_copy(n):
        dl, dz, dc = readers[n]
        return pltpu.make_async_remote_copy(
            src_ref=stats, dst_ref=statbuf.at[H, dl, dz], send_sem=send_sem.at[stat_s + n],
            recv_sem=recv_sem.at[stat_r + 8 * H + 4 * dl + dz], device_id=reader(dl, dz, dc), device_id_type=MESH,
        )

    for n, r in enumerate(readers):
        unless(straight, r == (0, 0, 0), lambda: stat_copy(n).start())

    x_r = sems("r", 4)
    x_s = sems("s", 4)

    first, second = pl.ds(0, half), pl.ds(half, half)
    halves = (first, second)

    def token_copy(b, n):
        return pltpu.make_async_remote_copy(
            src_ref=tok.at[halves[n]], dst_ref=xraw.at[L, halves[n]], send_sem=send_sem.at[x_s + 2 * b + n],
            recv_sem=recv_sem.at[x_r + 2 * L + n], device_id={"H": C, "L": b, "C": H}, device_id_type=MESH,
        )

    for b in (1 - L, L):
        mine = jnp.logical_and(straight, L == b)

        @pl.when(jnp.logical_not(mine))
        def _():
            for n in range(2):
                token_copy(b, n).start()

    send_w1(0, near[0])

    @pl.when(straight)
    def _():
        xraw[L] = tok[...]
        statbuf[H, 0, 0] = stats[...]

    yp_r, ym_r, far_r, sib_r = sems("r", 4), sems("r", 4), sems("r"), sems("r", 4)

    def to_sib(rel, b):
        copy(xbuf.at[C, rel, b], xbuf.at[C, rel, b], sib_r + rel, sib, "core")

    early = lax.rem(L + swapped, 2)

    def start_y(b):
        mine = jnp.logical_and(straight, L == b)
        dl = lax.rem(L + b, 2)

        @pl.when(jnp.logical_not(mine))
        def _():
            arrive(statbuf.at[H, dl, 0], stat_r + 8 * H + 4 * dl)

        arrive(statbuf.at[1 - H, dl, 0], stat_r + 8 * (1 - H) + 4 * dl)
        for src in range(2):
            for dz in range(1, 4):
                arrive(statbuf.at[src, dl, dz], stat_r + 8 * src + 4 * dl + dz)
        summed = statbuf[0, dl, 0]
        for src, dz in [(0, 1), (0, 2), (0, 3), (1, 0), (1, 1), (1, 2), (1, 3)]:
            summed = summed + statbuf[src, dl, dz]
        column = jnp.transpose(jnp.concatenate([summed] * 16, axis=0))
        mean = column[:, 0:1] / width
        spread = column[:, 1:2] / width - mean * mean
        scale = lax.rsqrt(spread + EPS)
        gains = jnp.concatenate([statbuf[C, dl, 0, pl.ds(2 + k, 1)] for k in range(feat // rows)], axis=1)

        for n, part in enumerate(halves):

            @pl.when(jnp.logical_not(mine))
            def _():
                arrive(xraw.at[b, part], x_r + 2 * b + n)

            at = slice(n * half, (n + 1) * half)
            xbuf[C, 0, b, part] = ((xraw[b, part].astype(F32) - mean[at]) * scale[at] * gains).astype(BF16)
            copy(xbuf.at[C, 0, b, part], xbuf.at[C, 3, b, part], yp_r + 2 * b + n, up, "y")
            copy(xbuf.at[C, 0, b, part], xbuf.at[C, 1, b, part], ym_r + 2 * b + n, down, "y")
        to_sib(0, b)

    def relay_y(b):
        arrive(xbuf.at[C, 3, b, first], yp_r + 2 * b)
        copy(xbuf.at[C, 3, b, first], xbuf.at[C, 2, b, first], far_r, up, "y")
        arrive(xbuf.at[C, 1, b, first], ym_r + 2 * b)
        arrive(xbuf.at[C, 1, b, second], ym_r + 2 * b + 1)
        copy(xbuf.at[C, 1, b, second], xbuf.at[C, 2, b, second], far_r, down, "y")
        to_sib(1, b)
        arrive(xbuf.at[C, 3, b, second], yp_r + 2 * b + 1)
        to_sib(3, b)

    def far_y():
        arrive(xbuf.at[C, 2], far_r)
        for b in range(2):
            to_sib(2, b)

    start_y(early)
    start_y(1 - early)
    send_w1(0, near[1])
    for j in range(1, CHUNKS):
        for dev in near:
            send_w1(j, dev)
    for f in range(PARTS):
        for dev in near:
            send_w2(f, dev)

    n_items = 4 * CHUNKS
    r1_r, r2_r = sems("r", n_items), sems("r", n_items)
    near_r, far_h = sems("r", 8), sems("r", 4)
    e_r = sems("r", 4 * PARTS)
    zp, zm, z2 = lax.rem(Z + 1, 4), lax.rem(Z + 3, 4), lax.rem(Z + 2, 4)
    seen_w, seen_x = set(), set()

    def s1(j, rel):
        i = 4 * j + rel
        if j not in seen_w:
            seen_w.add(j)
            arrive(w1buf.at[j], w1_r + j)
        if rel not in seen_x:
            seen_x.add(rel)
            arrive(xbuf.at[1 - C, rel], sib_r + rel)

        @pl.loop(0, 2)
        def _(b):
            features = jnp.concatenate([xbuf[0, rel, b], xbuf[1, rel, b]], axis=1)
            weights = w1buf[j].reshape(2 * feat, WIDE)
            acc = jnp.dot(features, weights, preferred_element_type=F32)
            pbuf[i, b] = acc[:, :HEAD_DIM].astype(BF16)
            pbuf[i, 2 + b] = acc[:, HEAD_DIM:].astype(BF16)

        copy(pbuf.at[i, z2, pl.ds(0, half)], r1.at[0, i], r1_r + i, fwd, "r1")
        copy(pbuf.at[i, z2, pl.ds(half, half)], r1.at[1, i], r1_r + i, back, "r1")

    def s2(j, rel):
        i = 4 * j + rel
        arrive(r1.at[:, i], r1_r + i)
        pbuf[i, zp, pl.ds(0, half)] = (pbuf[i, zp, pl.ds(0, half)].astype(F32) + r1[0, i].astype(F32)).astype(BF16)
        copy(pbuf.at[i, zp], r2.at[0, i], r2_r + i, fwd, "r2")
        pbuf[i, zm, pl.ds(half, half)] = (
            pbuf[i, zm, pl.ds(half, half)].astype(F32) + r1[1, i].astype(F32)
        ).astype(BF16)
        copy(pbuf.at[i, zm], r2.at[1, i], r2_r + i, back, "r2")

    def s3(j, rel):
        i = 4 * j + rel
        arrive(r2.at[:, i], r2_r + i)
        whole = (pbuf[i, Z].astype(F32) + r2[0, i].astype(F32) + r2[1, i].astype(F32)).astype(BF16)
        if j < 3:
            qkv[rel, j] = whole
        if j == 2:
            query = (head_norm(qkv[rel, 0].astype(F32)) * (1.0 / HEAD_DIM) ** 0.5).astype(BF16)
            keys = head_norm(qkv[rel, 1].astype(F32)).astype(BF16)
            scores = lax.dot_general(query, keys, (((1,), (1,)), ((), ())), preferred_element_type=F32)
            weights = jnp.exp(scores)
            probs = (weights / jnp.sum(weights, axis=-1, keepdims=True)).astype(BF16)
            hbuf[rel, Z, 0] = jnp.dot(probs, whole, preferred_element_type=F32).astype(BF16)
        if j >= 3:
            hbuf[rel, Z, j - 2] = gelu(whole.astype(F32)).astype(BF16)
        if j in (3, 5):
            k = (j - 3) // 2
            mine = hbuf.at[rel, Z, pl.ds(2 * k, 2)]
            copy(mine, mine, near_r + 2 * rel + k, fwd, "near")
            copy(mine, mine, near_r + 2 * rel + k, back, "near")

    def relay(k, rel):
        arrive(hbuf.at[rel, pl.ds(0, 2), pl.ds(2 * k, 2)], near_r + 2 * rel + k)
        top = hbuf.at[rel, zm, pl.ds(2 * k, 2), pl.ds(0, half)]
        copy(top, top, far_h + rel, fwd, "far")
        low = hbuf.at[rel, zp, pl.ds(2 * k, 2), pl.ds(half, half)]
        copy(low, low, far_h + rel, back, "far")

    seen_w2, seen_h = set(), set()

    def e1(f, rel):
        if f not in seen_w2:
            seen_w2.add(f)
            arrive(w2buf.at[:, f], w2_r + f)
        if rel not in seen_h:
            seen_h.add(rel)
            arrive(hbuf.at[rel, z2], far_h + rel)

        @pl.loop(0, 2)
        def _(b):
            hidden = jnp.concatenate([hbuf[rel, 2 * h + b, k] for k in range(4) for h in range(2)], axis=1)
            both = jnp.concatenate([w2buf[0, f], w2buf[1, f]], axis=1)
            whole = jnp.dot(hidden, both, preferred_element_type=F32).astype(BF16)
            for side in range(2):
                oall[side, rel, f, b] = whole[:, side * WIDE : (side + 1) * WIDE]

        copy(oall.at[1 - C, rel, f], osib.at[rel, f], e_r + rel * PARTS + f, sib, "cores")

    ry_r = sems("r", 3 * PARTS)
    xr_r = sems("r", 2 * PARTS)
    xr_s = sems("s", 2 * PARTS)

    def final_copy(b, f):
        return pltpu.make_async_remote_copy(
            src_ref=xsend.at[f, b], dst_ref=xrecv.at[f, L], send_sem=send_sem.at[xr_s + 2 * f + b],
            recv_sem=recv_sem.at[xr_r + 2 * f + L], device_id={"H": C, "L": b, "C": H}, device_id_type=MESH,
        )

    def e2(f, rel):
        arrive(osib.at[rel, f], e_r + rel * PARTS + f)
        ry = ry_r + 3 * f
        for b in range(2):
            total = oall[C, rel, f, b].astype(F32) + osib[rel, f, b].astype(F32)
            if rel == 1 and b == 0:
                arrive(ry1.at[f, 0], ry)
                total = total + ry1[f, 0].astype(F32)
            if rel == 3 and b == 1:
                arrive(ry1.at[f, 1], ry + 1)
                total = total + ry1[f, 1].astype(F32)
            if rel == 0:
                if b == 0:
                    arrive(ry2.at[f], ry + 2)
                xsend[f, b] = (total + ry2[f, 0, b].astype(F32) + ry2[f, 1, b].astype(F32)).astype(BF16)
                mine = jnp.logical_and(C == H, L == b)

                @pl.when(mine)
                def _():
                    xrecv[f, b] = xsend[f, b]

                @pl.when(jnp.logical_not(mine))
                def _():
                    final_copy(b, f).start()
            else:
                oall[C, rel, f, b] = total.astype(BF16)
        if rel == 2:
            copy(oall.at[C, 2, f, 0], ry1.at[f, 0], ry, up, "ry1")
            copy(oall.at[C, 2, f, 1], ry1.at[f, 1], ry + 1, down, "ry1")
        if rel == 1:
            copy(oall.at[C, 1, f], ry2.at[f, 0], ry + 2, up, "ry2")
        if rel == 3:
            copy(oall.at[C, 3, f], ry2.at[f, 1], ry + 2, down, "ry2")

    stages = {
        "y1": lambda a, rel: relay_y(early),
        "y2": lambda a, rel: relay_y(1 - early),
        "y3": lambda a, rel: far_y(),
        "s1": s1, "s2": s2, "s3": s3, "s4": relay, "e1": e1, "e2": e2,
    }
    for stage, a, rel in ORDER:
        stages[stage](a, rel)

    for f in range(PARTS):
        for b in range(2):

            @pl.when(jnp.logical_not(jnp.logical_and(C == H, L == b)))
            def _():
                arrive(xrecv.at[f, b], xr_r + 2 * f + b)

        columns = pl.ds(f * WIDE, WIDE)
        out[:, columns] = (
            tok[:, columns].astype(F32) + xrecv[f, 0].astype(F32) + xrecv[f, 1].astype(F32)
        ).astype(BF16)

    for n, r in enumerate(readers):
        unless(straight, r == (0, 0, 0), lambda: stat_copy(n).wait_send())
    whole = {
        "w1": w1buf, "w2": w2buf, "y": xbuf.at[0, pl.ds(0, 3)], "core": xbuf.at[0], "r1": r1, "r2": r2,
        "near": hbuf.at[pl.ds(0, 2)], "far": hbuf.at[0], "cores": osib, "ry1": ry1, "ry2": ry2,
    }
    for kind, (sem, total) in pending.items():
        ref = whole[kind]
        assert size(ref) == total, kind
        pltpu.make_async_remote_copy(
            src_ref=ref, dst_ref=ref, send_sem=send_sem.at[sem], recv_sem=recv_sem.at[0],
            device_id=sib, device_id_type=MESH,
        ).wait_send()
    for b in range(2):

        @pl.when(jnp.logical_not(jnp.logical_and(C == H, L == b)))
        def _():
            for n in range(2):
                token_copy(b, n).wait_send()

        @pl.when(jnp.logical_not(jnp.logical_and(C == H, L == b)))
        def _():
            for f in range(PARTS):
                final_copy(b, f).wait_send()

    assert count["s"] <= N_SEND and count["r"] <= N_RECV, count


def local(tokens, norm_gain, w_qkv, w_up, w_attn_out, w_down):
    rows, feat = tokens.shape
    width = feat * lax.axis_size("H") * lax.axis_size("Z")
    n_items = 4 * CHUNKS
    half = rows // 2
    vmem = pltpu.VMEM
    out_part = (PARTS, 2, rows, WIDE)
    scratch = [
        vmem((8, rows), F32),
        vmem((2, 2, 4, 8, rows), F32),
        vmem((2, rows, feat), BF16),
        vmem((2, 4, 2, rows, feat), BF16),
        vmem((CHUNKS, 2, feat, WIDE), BF16),
        vmem((2, PARTS, w_attn_out.shape[0] + w_down.shape[0], WIDE), BF16),
        vmem((n_items, 4, rows, HEAD_DIM), BF16),
        vmem((2, n_items, half, HEAD_DIM), BF16),
        vmem((2, n_items, rows, HEAD_DIM), BF16),
        vmem((4, 3, rows, HEAD_DIM), BF16),
        vmem((4, 4, 4, rows, HEAD_DIM), BF16),
        vmem((2, 4, *out_part), BF16),
        vmem((4, *out_part), BF16),
        vmem((PARTS, 2, rows, WIDE), BF16),
        vmem((PARTS, 2, 2, rows, WIDE), BF16),
        vmem(out_part, BF16),
        vmem(out_part, BF16),
        pltpu.SemaphoreType.DMA((N_SEND,)),
        pltpu.SemaphoreType.DMA((N_RECV,)),
    ]
    in_vmem = pl.BlockSpec(memory_space=pltpu.VMEM)
    anywhere = pl.BlockSpec(memory_space=pl.ANY)
    return pl.pallas_call(
        functools.partial(kernel, width),
        out_shape=jax.ShapeDtypeStruct((rows, feat), BF16),
        in_specs=[in_vmem] * 2 + [anywhere] * 4,
        out_specs=in_vmem,
        scratch_shapes=scratch,
        compiler_params=pltpu.CompilerParams(
            collective_id=0, has_side_effects=True, vmem_limit_bytes=60 * 1024 * 1024
        ),
        name="layer",
    )(tokens, norm_gain, w_qkv.transpose(1, 0, 2), w_up, w_attn_out, w_down)


def solution(mesh):
    torus = Mesh(mesh.devices.reshape(2, 4, 2, 2, 4), ("L", "Y", "C", "H", "Z"))
    in_specs = (P(DP, MP), P(MP), P(MP, None, DP), P(MP, DP), P(DP, MP), P(DP, MP))
    return jax.shard_map(local, mesh=torus, in_specs=in_specs, out_specs=P(DP, MP), check_vma=False)
```

```python
import functools
import math

import jax
import jax.numpy as jnp
from jax import lax
from jax.experimental import pallas as pl
from jax.experimental.pallas import tpu as pltpu
from jax.sharding import Mesh
from jax.sharding import PartitionSpec as P

HEAD_DIM = 128
PATCHES = 256
EPS = 1e-06
MESH = pl.DeviceIdType.MESH
F32 = jnp.float32
BF16 = jnp.bfloat16
DP = ("L", "Y", "C")
MP = ("H", "Z")

CHUNKS = 6
WIDE = 2 * HEAD_DIM
PARTS = 3
ORDER = (
    ("y1", 0, 0), ("s1", 0, 0), ("y2", 0, 0), ("s2", 0, 0), ("s1", 1, 0), ("s1", 0, 1), ("s1", 1, 3), ("s1", 1, 1),
    ("s2", 1, 0), ("s1", 0, 3), ("s2", 0, 1), ("s2", 1, 3), ("s1", 2, 3), ("y3", 0, 0), ("s2", 1, 1), ("s2", 0, 3),
    ("s1", 2, 2), ("s2", 2, 3), ("s1", 1, 2), ("s1", 0, 2), ("s1", 2, 1), ("s2", 2, 2), ("s3", 0, 1), ("s1", 3, 3),
    ("s1", 3, 2), ("s3", 1, 1), ("s1", 3, 1), ("s2", 0, 2), ("s2", 2, 1), ("s2", 1, 2), ("s2", 3, 1), ("s2", 3, 3),
    ("s1", 4, 1), ("s3", 0, 3), ("s1", 4, 2), ("s3", 0, 2), ("s1", 4, 3), ("s3", 1, 2), ("s3", 2, 1), ("s1", 2, 0),
    ("s3", 3, 1), ("s2", 3, 2), ("s3", 2, 2), ("s2", 4, 3), ("s1", 5, 1), ("s1", 5, 2), ("s2", 4, 2), ("s3", 3, 2),
    ("s3", 1, 3), ("s3", 2, 3), ("s2", 5, 2), ("s2", 5, 1), ("s3", 3, 3), ("s4", 0, 2), ("s2", 4, 1), ("s1", 5, 3),
    ("s3", 4, 2), ("s3", 5, 2), ("s1", 4, 0), ("s1", 5, 0), ("s1", 3, 0), ("s2", 5, 3), ("s3", 4, 1), ("s3", 5, 1),
    ("s4", 1, 2), ("s3", 4, 3), ("s3", 5, 3), ("s4", 1, 1), ("s4", 0, 1), ("s3", 0, 0), ("s4", 0, 3), ("e1", 1, 2),
    ("s4", 1, 3), ("e2", 1, 2), ("e1", 0, 2), ("s2", 2, 0), ("e1", 2, 2), ("s2", 3, 0), ("s2", 4, 0), ("s2", 5, 0),
    ("s3", 1, 0), ("e2", 0, 2), ("e1", 0, 1), ("e1", 1, 1), ("e2", 2, 2), ("e1", 0, 3), ("e1", 2, 1), ("s3", 2, 0),
    ("s3", 3, 0), ("e2", 1, 1), ("e2", 0, 1), ("e2", 0, 3), ("s3", 4, 0), ("s3", 5, 0), ("e1", 1, 3), ("e1", 2, 3),
    ("e2", 1, 3), ("s4", 0, 0), ("e2", 2, 1), ("s4", 1, 0), ("e2", 2, 3), ("e1", 1, 0), ("e2", 1, 0), ("e1", 0, 0),
    ("e2", 0, 0), ("e1", 2, 0), ("e2", 2, 0),
)
N_SEND = 37
N_RECV = 129


def gelu(u):
    return 0.5 * u * (1.0 + jnp.tanh(0.7978845608028654 * (u + 0.044715 * (u * u * u))))


def head_norm(values):
    mean = jnp.mean(values, axis=-1, keepdims=True)
    centered = values - mean
    spread = jnp.mean(centered * centered, axis=-1, keepdims=True)
    return centered * lax.rsqrt(spread + EPS)


def kernel(
    width,
    tok, gain, w_qkv, w_up, w_attn, w_down,
    out,
    stats, statbuf, xraw, xbuf, w1buf, w2buf, pbuf, r1, r2, qkv, hbuf, oall, osib, ry1, ry2, xsend, xrecv,
    send_sem, recv_sem,
):
    L, Y, C, H, Z = (lax.axis_index(a) for a in ("L", "Y", "C", "H", "Z"))
    rows, feat = tok.shape
    half = rows // 2
    near = ({"L": 1 - L, "H": C}, {"L": 1 - L, "H": 1 - C})
    up, down = {"Y": lax.rem(Y + 1, 4)}, {"Y": lax.rem(Y + 3, 4)}
    fwd, back = {"Z": lax.rem(Z + 1, 4)}, {"Z": lax.rem(Z + 3, 4)}
    sib = {"C": 1 - C}
    swapped = (C != H).astype(jnp.int32)
    straight = C == H

    count = {"s": 0, "r": 0}
    pending = {}

    def sems(kind, n=1):
        first = count[kind]
        count[kind] += n
        return first

    def size(ref):
        return math.prod(ref.shape) * 2

    def copy(src, dst, recv, dev, kind):
        if kind not in pending:
            pending[kind] = [sems("s"), 0]
        pending[kind][1] += size(src)
        pltpu.make_async_remote_copy(
            src_ref=src, dst_ref=dst, send_sem=send_sem.at[pending[kind][0]], recv_sem=recv_sem.at[recv],
            device_id=dev, device_id_type=MESH,
        ).start()

    def arrive(dst, recv):
        pltpu.make_async_remote_copy(
            src_ref=dst, dst_ref=dst, send_sem=send_sem.at[0], recv_sem=recv_sem.at[recv],
            device_id=sib, device_id_type=MESH,
        ).wait_recv()

    barrier = pltpu.get_barrier_semaphore()
    for dev in (*near, up, down, fwd, back, sib):
        pl.semaphore_signal(barrier, inc=1, device_id=dev, device_id_type=MESH)

    readers = [(dl, dz, dc) for dl in range(2) for dz in range(4) for dc in range(2)]

    def reader(dl, dz, dc):
        return {"H": C, "L": lax.rem(L + dl, 2), "Z": lax.rem(Z + dz, 4), "C": lax.rem(C + dc, 2)}

    def unless(condition, skip, f):
        if skip:
            pl.when(jnp.logical_not(condition))(f)
        else:
            f()

    for dh, dl, dz in [(dh, dl, dz) for dh in range(2) for dl in range(2) for dz in range(4)]:

        def greet():
            source = {"C": H, "H": lax.rem(H + dh, 2), "L": lax.rem(L + dl, 2), "Z": lax.rem(Z + dz, 4)}
            pl.semaphore_signal(barrier, inc=1, device_id=source, device_id_type=MESH)

        unless(straight, dh + dl + dz == 0, greet)

    w1_r = sems("r", CHUNKS)
    w2_r = sems("r", PARTS)

    def send_w1(j, dev):
        block = w_qkv.at[j] if j < 3 else w_up.at[:, pl.ds((j - 3) * WIDE, WIDE)]
        copy(block, w1buf.at[j, H], w1_r + j, dev, "w1")

    def send_w2(f, dev):
        top, columns = w_attn.shape[0], pl.ds(f * WIDE, WIDE)
        copy(w_attn.at[:, columns], w2buf.at[H, f, pl.ds(0, top)], w2_r + f, dev, "w2")
        copy(w_down.at[:, columns], w2buf.at[H, f, pl.ds(top, w_down.shape[0])], w2_r + f, dev, "w2")

    tokens_f = tok[...].astype(F32)
    lane = lax.broadcasted_iota(jnp.int32, (rows, 128), 1)
    total = jnp.sum(tokens_f, axis=1, keepdims=True)
    squares = jnp.sum(tokens_f * tokens_f, axis=1, keepdims=True)
    stats[...] = jnp.transpose(jnp.where(lane == 0, total, jnp.where(lane == 1, squares, 0.0)))[0:8]
    for k in range(feat // rows):
        stats[pl.ds(2 + k, 1)] = gain[pl.ds(k * rows, rows)][None, :]

    pl.semaphore_wait(barrier, 23 - straight.astype(jnp.int32))

    stat_r = sems("r", 16)
    stat_s = sems("s", 16)

    def stat_copy(n):
        dl, dz, dc = readers[n]
        return pltpu.make_async_remote_copy(
            src_ref=stats, dst_ref=statbuf.at[H, dl, dz], send_sem=send_sem.at[stat_s + n],
            recv_sem=recv_sem.at[stat_r + 8 * H + 4 * dl + dz], device_id=reader(dl, dz, dc), device_id_type=MESH,
        )

    for n, r in enumerate(readers):
        unless(straight, r == (0, 0, 0), lambda: stat_copy(n).start())

    x_r = sems("r", 4)
    x_s = sems("s", 4)

    first, second = pl.ds(0, half), pl.ds(half, half)
    halves = (first, second)

    def token_copy(b, n):
        return pltpu.make_async_remote_copy(
            src_ref=tok.at[halves[n]], dst_ref=xraw.at[L, halves[n]], send_sem=send_sem.at[x_s + 2 * b + n],
            recv_sem=recv_sem.at[x_r + 2 * L + n], device_id={"H": C, "L": b, "C": H}, device_id_type=MESH,
        )

    for b in (1 - L, L):
        mine = jnp.logical_and(straight, L == b)

        @pl.when(jnp.logical_not(mine))
        def _():
            for n in range(2):
                token_copy(b, n).start()

    send_w1(0, near[0])

    @pl.when(straight)
    def _():
        xraw[L] = tok[...]
        statbuf[H, 0, 0] = stats[...]

    yp_r, ym_r, far_r, sib_r = sems("r", 4), sems("r", 4), sems("r"), sems("r", 4)

    def to_sib(rel, b):
        copy(xbuf.at[C, rel, b], xbuf.at[C, rel, b], sib_r + rel, sib, "core")

    early = lax.rem(L + swapped, 2)

    def start_y(b):
        mine = jnp.logical_and(straight, L == b)
        dl = lax.rem(L + b, 2)

        @pl.when(jnp.logical_not(mine))
        def _():
            arrive(statbuf.at[H, dl, 0], stat_r + 8 * H + 4 * dl)

        arrive(statbuf.at[1 - H, dl, 0], stat_r + 8 * (1 - H) + 4 * dl)
        for src in range(2):
            for dz in range(1, 4):
                arrive(statbuf.at[src, dl, dz], stat_r + 8 * src + 4 * dl + dz)
        summed = statbuf[0, dl, 0]
        for src, dz in [(0, 1), (0, 2), (0, 3), (1, 0), (1, 1), (1, 2), (1, 3)]:
            summed = summed + statbuf[src, dl, dz]
        column = jnp.transpose(jnp.concatenate([summed] * 16, axis=0))
        mean = column[:, 0:1] / width
        spread = column[:, 1:2] / width - mean * mean
        scale = lax.rsqrt(spread + EPS)
        gains = jnp.concatenate([statbuf[C, dl, 0, pl.ds(2 + k, 1)] for k in range(feat // rows)], axis=1)

        for n, part in enumerate(halves):

            @pl.when(jnp.logical_not(mine))
            def _():
                arrive(xraw.at[b, part], x_r + 2 * b + n)

            at = slice(n * half, (n + 1) * half)
            xbuf[C, 0, b, part] = ((xraw[b, part].astype(F32) - mean[at]) * scale[at] * gains).astype(BF16)
            copy(xbuf.at[C, 0, b, part], xbuf.at[C, 3, b, part], yp_r + 2 * b + n, up, "y")
            copy(xbuf.at[C, 0, b, part], xbuf.at[C, 1, b, part], ym_r + 2 * b + n, down, "y")
        to_sib(0, b)

    def relay_y(b):
        arrive(xbuf.at[C, 3, b, first], yp_r + 2 * b)
        copy(xbuf.at[C, 3, b, first], xbuf.at[C, 2, b, first], far_r, up, "y")
        arrive(xbuf.at[C, 1, b, first], ym_r + 2 * b)
        arrive(xbuf.at[C, 1, b, second], ym_r + 2 * b + 1)
        copy(xbuf.at[C, 1, b, second], xbuf.at[C, 2, b, second], far_r, down, "y")
        to_sib(1, b)
        arrive(xbuf.at[C, 3, b, second], yp_r + 2 * b + 1)
        to_sib(3, b)

    def far_y():
        arrive(xbuf.at[C, 2], far_r)
        for b in range(2):
            to_sib(2, b)

    start_y(early)
    start_y(1 - early)
    send_w1(0, near[1])
    for j in range(1, CHUNKS):
        for dev in near:
            send_w1(j, dev)
    for f in range(PARTS):
        for dev in near:
            send_w2(f, dev)

    n_items = 4 * CHUNKS
    r1_r, r2_r = sems("r", n_items), sems("r", n_items)
    near_r, far_h = sems("r", 8), sems("r", 4)
    e_r = sems("r", 4 * PARTS)
    zp, zm, z2 = lax.rem(Z + 1, 4), lax.rem(Z + 3, 4), lax.rem(Z + 2, 4)
    seen_w, seen_x = set(), set()

    def s1(j, rel):
        i = 4 * j + rel
        if j not in seen_w:
            seen_w.add(j)
            arrive(w1buf.at[j], w1_r + j)
        if rel not in seen_x:
            seen_x.add(rel)
            arrive(xbuf.at[1 - C, rel], sib_r + rel)

        @pl.loop(0, 2)
        def _(b):
            features = jnp.concatenate([xbuf[0, rel, b], xbuf[1, rel, b]], axis=1)
            weights = w1buf[j].reshape(2 * feat, WIDE)
            acc = jnp.dot(features, weights, preferred_element_type=F32)
            pbuf[i, b] = acc[:, :HEAD_DIM].astype(BF16)
            pbuf[i, 2 + b] = acc[:, HEAD_DIM:].astype(BF16)

        copy(pbuf.at[i, z2, pl.ds(0, half)], r1.at[0, i], r1_r + i, fwd, "r1")
        copy(pbuf.at[i, z2, pl.ds(half, half)], r1.at[1, i], r1_r + i, back, "r1")

    def s2(j, rel):
        i = 4 * j + rel
        arrive(r1.at[:, i], r1_r + i)
        pbuf[i, zp, pl.ds(0, half)] = (pbuf[i, zp, pl.ds(0, half)].astype(F32) + r1[0, i].astype(F32)).astype(BF16)
        copy(pbuf.at[i, zp], r2.at[0, i], r2_r + i, fwd, "r2")
        pbuf[i, zm, pl.ds(half, half)] = (
            pbuf[i, zm, pl.ds(half, half)].astype(F32) + r1[1, i].astype(F32)
        ).astype(BF16)
        copy(pbuf.at[i, zm], r2.at[1, i], r2_r + i, back, "r2")

    def s3(j, rel):
        i = 4 * j + rel
        arrive(r2.at[:, i], r2_r + i)
        whole = (pbuf[i, Z].astype(F32) + r2[0, i].astype(F32) + r2[1, i].astype(F32)).astype(BF16)
        if j < 3:
            qkv[rel, j] = whole
        if j == 2:
            query = (head_norm(qkv[rel, 0].astype(F32)) * (1.0 / HEAD_DIM) ** 0.5).astype(BF16)
            keys = head_norm(qkv[rel, 1].astype(F32)).astype(BF16)
            scores = lax.dot_general(query, keys, (((1,), (1,)), ((), ())), preferred_element_type=F32)
            weights = jnp.exp(scores)
            probs = (weights / jnp.sum(weights, axis=-1, keepdims=True)).astype(BF16)
            hbuf[rel, Z, 0] = jnp.dot(probs, whole, preferred_element_type=F32).astype(BF16)
        if j >= 3:
            hbuf[rel, Z, j - 2] = gelu(whole.astype(F32)).astype(BF16)
        if j in (3, 5):
            k = (j - 3) // 2
            mine = hbuf.at[rel, Z, pl.ds(2 * k, 2)]
            copy(mine, mine, near_r + 2 * rel + k, fwd, "near")
            copy(mine, mine, near_r + 2 * rel + k, back, "near")

    def relay(k, rel):
        arrive(hbuf.at[rel, pl.ds(0, 2), pl.ds(2 * k, 2)], near_r + 2 * rel + k)
        top = hbuf.at[rel, zm, pl.ds(2 * k, 2), pl.ds(0, half)]
        copy(top, top, far_h + rel, fwd, "far")
        low = hbuf.at[rel, zp, pl.ds(2 * k, 2), pl.ds(half, half)]
        copy(low, low, far_h + rel, back, "far")

    seen_w2, seen_h = set(), set()

    def e1(f, rel):
        if f not in seen_w2:
            seen_w2.add(f)
            arrive(w2buf.at[:, f], w2_r + f)
        if rel not in seen_h:
            seen_h.add(rel)
            arrive(hbuf.at[rel, z2], far_h + rel)

        @pl.loop(0, 2)
        def _(b):
            hidden = jnp.concatenate([hbuf[rel, 2 * h + b, k] for k in range(4) for h in range(2)], axis=1)
            both = jnp.concatenate([w2buf[0, f], w2buf[1, f]], axis=1)
            whole = jnp.dot(hidden, both, preferred_element_type=F32).astype(BF16)
            for side in range(2):
                oall[side, rel, f, b] = whole[:, side * WIDE : (side + 1) * WIDE]

        copy(oall.at[1 - C, rel, f], osib.at[rel, f], e_r + rel * PARTS + f, sib, "cores")

    ry_r = sems("r", 3 * PARTS)
    xr_r = sems("r", 2 * PARTS)
    xr_s = sems("s", 2 * PARTS)

    def final_copy(b, f):
        return pltpu.make_async_remote_copy(
            src_ref=xsend.at[f, b], dst_ref=xrecv.at[f, L], send_sem=send_sem.at[xr_s + 2 * f + b],
            recv_sem=recv_sem.at[xr_r + 2 * f + L], device_id={"H": C, "L": b, "C": H}, device_id_type=MESH,
        )

    def e2(f, rel):
        arrive(osib.at[rel, f], e_r + rel * PARTS + f)
        ry = ry_r + 3 * f
        for b in range(2):
            total = oall[C, rel, f, b].astype(F32) + osib[rel, f, b].astype(F32)
            if rel == 1 and b == 0:
                arrive(ry1.at[f, 0], ry)
                total = total + ry1[f, 0].astype(F32)
            if rel == 3 and b == 1:
                arrive(ry1.at[f, 1], ry + 1)
                total = total + ry1[f, 1].astype(F32)
            if rel == 0:
                if b == 0:
                    arrive(ry2.at[f], ry + 2)
                xsend[f, b] = (total + ry2[f, 0, b].astype(F32) + ry2[f, 1, b].astype(F32)).astype(BF16)
                mine = jnp.logical_and(C == H, L == b)

                @pl.when(mine)
                def _():
                    xrecv[f, b] = xsend[f, b]

                @pl.when(jnp.logical_not(mine))
                def _():
                    final_copy(b, f).start()
            else:
                oall[C, rel, f, b] = total.astype(BF16)
        if rel == 2:
            copy(oall.at[C, 2, f, 0], ry1.at[f, 0], ry, up, "ry1")
            copy(oall.at[C, 2, f, 1], ry1.at[f, 1], ry + 1, down, "ry1")
        if rel == 1:
            copy(oall.at[C, 1, f], ry2.at[f, 0], ry + 2, up, "ry2")
        if rel == 3:
            copy(oall.at[C, 3, f], ry2.at[f, 1], ry + 2, down, "ry2")

    stages = {
        "y1": lambda a, rel: relay_y(early),
        "y2": lambda a, rel: relay_y(1 - early),
        "y3": lambda a, rel: far_y(),
        "s1": s1, "s2": s2, "s3": s3, "s4": relay, "e1": e1, "e2": e2,
    }
    for stage, a, rel in ORDER:
        stages[stage](a, rel)

    for f in range(PARTS):
        for b in range(2):

            @pl.when(jnp.logical_not(jnp.logical_and(C == H, L == b)))
            def _():
                arrive(xrecv.at[f, b], xr_r + 2 * f + b)

        columns = pl.ds(f * WIDE, WIDE)
        out[:, columns] = (
            tok[:, columns].astype(F32) + xrecv[f, 0].astype(F32) + xrecv[f, 1].astype(F32)
        ).astype(BF16)

    for n, r in enumerate(readers):
        unless(straight, r == (0, 0, 0), lambda: stat_copy(n).wait_send())
    whole = {
        "w1": w1buf, "w2": w2buf, "y": xbuf.at[0, pl.ds(0, 3)], "core": xbuf.at[0], "r1": r1, "r2": r2,
        "near": hbuf.at[pl.ds(0, 2)], "far": hbuf.at[0], "cores": osib, "ry1": ry1, "ry2": ry2,
    }
    for kind, (sem, total) in pending.items():
        ref = whole[kind]
        assert size(ref) == total, kind
        pltpu.make_async_remote_copy(
            src_ref=ref, dst_ref=ref, send_sem=send_sem.at[sem], recv_sem=recv_sem.at[0],
            device_id=sib, device_id_type=MESH,
        ).wait_send()
    for b in range(2):

        @pl.when(jnp.logical_not(jnp.logical_and(C == H, L == b)))
        def _():
            for n in range(2):
                token_copy(b, n).wait_send()

        @pl.when(jnp.logical_not(jnp.logical_and(C == H, L == b)))
        def _():
            for f in range(PARTS):
                final_copy(b, f).wait_send()

    assert count["s"] <= N_SEND and count["r"] <= N_RECV, count


def local(tokens, norm_gain, w_qkv, w_up, w_attn_out, w_down):
    rows, feat = tokens.shape
    width = feat * lax.axis_size("H") * lax.axis_size("Z")
    n_items = 4 * CHUNKS
    half = rows // 2
    vmem = pltpu.VMEM
    out_part = (PARTS, 2, rows, WIDE)
    scratch = [
        vmem((8, rows), F32),
        vmem((2, 2, 4, 8, rows), F32),
        vmem((2, rows, feat), BF16),
        vmem((2, 4, 2, rows, feat), BF16),
        vmem((CHUNKS, 2, feat, WIDE), BF16),
        vmem((2, PARTS, w_attn_out.shape[0] + w_down.shape[0], WIDE), BF16),
        vmem((n_items, 4, rows, HEAD_DIM), BF16),
        vmem((2, n_items, half, HEAD_DIM), BF16),
        vmem((2, n_items, rows, HEAD_DIM), BF16),
        vmem((4, 3, rows, HEAD_DIM), BF16),
        vmem((4, 4, 4, rows, HEAD_DIM), BF16),
        vmem((2, 4, *out_part), BF16),
        vmem((4, *out_part), BF16),
        vmem((PARTS, 2, rows, WIDE), BF16),
        vmem((PARTS, 2, 2, rows, WIDE), BF16),
        vmem(out_part, BF16),
        vmem(out_part, BF16),
        pltpu.SemaphoreType.DMA((N_SEND,)),
        pltpu.SemaphoreType.DMA((N_RECV,)),
    ]
    in_vmem = pl.BlockSpec(memory_space=pltpu.VMEM)
    anywhere = pl.BlockSpec(memory_space=pl.ANY)
    return pl.pallas_call(
        functools.partial(kernel, width),
        out_shape=jax.ShapeDtypeStruct((rows, feat), BF16),
        in_specs=[in_vmem] * 2 + [anywhere] * 4,
        out_specs=in_vmem,
        scratch_shapes=scratch,
        compiler_params=pltpu.CompilerParams(
            collective_id=0, has_side_effects=True, vmem_limit_bytes=60 * 1024 * 1024
        ),
        name="layer",
    )(tokens, norm_gain, w_qkv.transpose(1, 0, 2), w_up, w_attn_out, w_down)


def solution(mesh):
    torus = Mesh(mesh.devices.reshape(2, 4, 2, 2, 4), ("L", "Y", "C", "H", "Z"))
    in_specs = (P(DP, MP), P(MP), P(MP, None, DP), P(MP, DP), P(DP, MP), P(DP, MP))
    return jax.shard_map(local, mesh=torus, in_specs=in_specs, out_specs=P(DP, MP), check_vma=False)
```

```python
import functools
import math

import jax
import jax.numpy as jnp
from jax import lax
from jax.experimental import pallas as pl
from jax.experimental.pallas import tpu as pltpu
from jax.sharding import Mesh
from jax.sharding import PartitionSpec as P

HEAD_DIM = 128
PATCHES = 256
EPS = 1e-06
MESH = pl.DeviceIdType.MESH
F32 = jnp.float32
BF16 = jnp.bfloat16
DP = ("L", "Y", "C")
MP = ("H", "Z")

CHUNKS = 6
WIDE = 2 * HEAD_DIM
PARTS = 3
ORDER = (
    ("y1", 0, 0), ("s1", 0, 0), ("y2", 0, 0), ("s2", 0, 0), ("s1", 1, 0), ("s1", 0, 1), ("s1", 1, 3), ("s1", 1, 1),
    ("s2", 1, 0), ("s1", 0, 3), ("s2", 0, 1), ("s2", 1, 3), ("s1", 2, 3), ("y3", 0, 0), ("s2", 1, 1), ("s2", 0, 3),
    ("s1", 2, 2), ("s2", 2, 3), ("s1", 1, 2), ("s1", 0, 2), ("s1", 2, 1), ("s2", 2, 2), ("s3", 0, 1), ("s1", 3, 3),
    ("s1", 3, 2), ("s3", 1, 1), ("s1", 3, 1), ("s2", 0, 2), ("s2", 2, 1), ("s2", 1, 2), ("s2", 3, 1), ("s2", 3, 3),
    ("s1", 4, 1), ("s3", 0, 3), ("s1", 4, 2), ("s3", 0, 2), ("s1", 4, 3), ("s3", 1, 2), ("s3", 2, 1), ("s1", 2, 0),
    ("s3", 3, 1), ("s2", 3, 2), ("s3", 2, 2), ("s2", 4, 3), ("s1", 5, 1), ("s1", 5, 2), ("s2", 4, 2), ("s3", 3, 2),
    ("s3", 1, 3), ("s3", 2, 3), ("s2", 5, 2), ("s2", 5, 1), ("s3", 3, 3), ("s4", 0, 2), ("s2", 4, 1), ("s1", 5, 3),
    ("s3", 4, 2), ("s3", 5, 2), ("s1", 4, 0), ("s1", 5, 0), ("s1", 3, 0), ("s2", 5, 3), ("s3", 4, 1), ("s3", 5, 1),
    ("s4", 1, 2), ("s3", 4, 3), ("s3", 5, 3), ("s4", 1, 1), ("s4", 0, 1), ("s3", 0, 0), ("s4", 0, 3), ("s4", 1, 3),
    ("e1", 1, 2), ("e2", 1, 2), ("e1", 0, 2), ("s2", 2, 0), ("e1", 2, 2), ("s2", 3, 0), ("s2", 4, 0), ("s2", 5, 0),
    ("s3", 1, 0), ("e2", 0, 2), ("e1", 0, 1), ("e1", 1, 1), ("e2", 2, 2), ("e1", 0, 3), ("e1", 2, 1), ("s3", 2, 0),
    ("s3", 3, 0), ("e2", 1, 1), ("e2", 0, 1), ("e2", 0, 3), ("s3", 4, 0), ("s3", 5, 0), ("e1", 1, 3), ("e1", 2, 3),
    ("e2", 1, 3), ("s4", 0, 0), ("e2", 2, 1), ("s4", 1, 0), ("e2", 2, 3), ("e1", 1, 0), ("e2", 1, 0), ("e1", 0, 0),
    ("e2", 0, 0), ("e1", 2, 0), ("e2", 2, 0),
)
N_SEND = 37
N_RECV = 129


def gelu(u):
    return 0.5 * u * (1.0 + jnp.tanh(0.7978845608028654 * (u + 0.044715 * (u * u * u))))


def head_norm(values):
    mean = jnp.mean(values, axis=-1, keepdims=True)
    centered = values - mean
    spread = jnp.mean(centered * centered, axis=-1, keepdims=True)
    return centered * lax.rsqrt(spread + EPS)


def kernel(
    width,
    tok, gain, w_qkv, w_up, w_attn, w_down,
    out,
    stats, statbuf, xraw, xbuf, w1buf, w2buf, pbuf, r1, r2, qkv, hbuf, oall, osib, ry1, ry2, xsend, xrecv,
    send_sem, recv_sem,
):
    L, Y, C, H, Z = (lax.axis_index(a) for a in ("L", "Y", "C", "H", "Z"))
    rows, feat = tok.shape
    half = rows // 2
    near = ({"L": 1 - L, "H": C}, {"L": 1 - L, "H": 1 - C})
    up, down = {"Y": lax.rem(Y + 1, 4)}, {"Y": lax.rem(Y + 3, 4)}
    fwd, back = {"Z": lax.rem(Z + 1, 4)}, {"Z": lax.rem(Z + 3, 4)}
    sib = {"C": 1 - C}
    swapped = (C != H).astype(jnp.int32)
    straight = C == H

    count = {"s": 0, "r": 0}
    pending = {}

    def sems(kind, n=1):
        first = count[kind]
        count[kind] += n
        return first

    def size(ref):
        return math.prod(ref.shape) * 2

    def copy(src, dst, recv, dev, kind):
        if kind not in pending:
            pending[kind] = [sems("s"), 0]
        pending[kind][1] += size(src)
        pltpu.make_async_remote_copy(
            src_ref=src, dst_ref=dst, send_sem=send_sem.at[pending[kind][0]], recv_sem=recv_sem.at[recv],
            device_id=dev, device_id_type=MESH,
        ).start()

    def arrive(dst, recv):
        pltpu.make_async_remote_copy(
            src_ref=dst, dst_ref=dst, send_sem=send_sem.at[0], recv_sem=recv_sem.at[recv],
            device_id=sib, device_id_type=MESH,
        ).wait_recv()

    barrier = pltpu.get_barrier_semaphore()
    for dev in (*near, up, down, fwd, back, sib):
        pl.semaphore_signal(barrier, inc=1, device_id=dev, device_id_type=MESH)

    readers = [(dl, dz, dc) for dl in range(2) for dz in range(4) for dc in range(2)]

    def reader(dl, dz, dc):
        return {"H": C, "L": lax.rem(L + dl, 2), "Z": lax.rem(Z + dz, 4), "C": lax.rem(C + dc, 2)}

    def unless(condition, skip, f):
        if skip:
            pl.when(jnp.logical_not(condition))(f)
        else:
            f()

    for dh, dl, dz in [(dh, dl, dz) for dh in range(2) for dl in range(2) for dz in range(4)]:

        def greet():
            source = {"C": H, "H": lax.rem(H + dh, 2), "L": lax.rem(L + dl, 2), "Z": lax.rem(Z + dz, 4)}
            pl.semaphore_signal(barrier, inc=1, device_id=source, device_id_type=MESH)

        unless(straight, dh + dl + dz == 0, greet)

    w1_r = sems("r", CHUNKS)
    w2_r = sems("r", PARTS)

    def send_w1(j, dev):
        block = w_qkv.at[j] if j < 3 else w_up.at[:, pl.ds((j - 3) * WIDE, WIDE)]
        copy(block, w1buf.at[j, H], w1_r + j, dev, "w1")

    def send_w2(f, dev):
        top, columns = w_attn.shape[0], pl.ds(f * WIDE, WIDE)
        copy(w_attn.at[:, columns], w2buf.at[H, f, pl.ds(0, top)], w2_r + f, dev, "w2")
        copy(w_down.at[:, columns], w2buf.at[H, f, pl.ds(top, w_down.shape[0])], w2_r + f, dev, "w2")

    tokens_f = tok[...].astype(F32)
    lane = lax.broadcasted_iota(jnp.int32, (rows, 128), 1)
    total = jnp.sum(tokens_f, axis=1, keepdims=True)
    squares = jnp.sum(tokens_f * tokens_f, axis=1, keepdims=True)
    stats[...] = jnp.transpose(jnp.where(lane == 0, total, jnp.where(lane == 1, squares, 0.0)))[0:8]
    for k in range(feat // rows):
        stats[pl.ds(2 + k, 1)] = gain[pl.ds(k * rows, rows)][None, :]

    pl.semaphore_wait(barrier, 23 - straight.astype(jnp.int32))

    stat_r = sems("r", 16)
    stat_s = sems("s", 16)

    def stat_copy(n):
        dl, dz, dc = readers[n]
        return pltpu.make_async_remote_copy(
            src_ref=stats, dst_ref=statbuf.at[H, dl, dz], send_sem=send_sem.at[stat_s + n],
            recv_sem=recv_sem.at[stat_r + 8 * H + 4 * dl + dz], device_id=reader(dl, dz, dc), device_id_type=MESH,
        )

    for n, r in enumerate(readers):
        unless(straight, r == (0, 0, 0), lambda: stat_copy(n).start())

    x_r = sems("r", 4)
    x_s = sems("s", 4)

    first, second = pl.ds(0, half), pl.ds(half, half)
    halves = (first, second)

    def token_copy(b, n):
        return pltpu.make_async_remote_copy(
            src_ref=tok.at[halves[n]], dst_ref=xraw.at[L, halves[n]], send_sem=send_sem.at[x_s + 2 * b + n],
            recv_sem=recv_sem.at[x_r + 2 * L + n], device_id={"H": C, "L": b, "C": H}, device_id_type=MESH,
        )

    for b in (1 - L, L):
        mine = jnp.logical_and(straight, L == b)

        @pl.when(jnp.logical_not(mine))
        def _():
            for n in range(2):
                token_copy(b, n).start()

    send_w1(0, near[0])

    @pl.when(straight)
    def _():
        xraw[L] = tok[...]
        statbuf[H, 0, 0] = stats[...]

    yp_r, ym_r, far_r, sib_r = sems("r", 4), sems("r", 4), sems("r"), sems("r", 4)

    def to_sib(rel, b):
        copy(xbuf.at[C, rel, b], xbuf.at[C, rel, b], sib_r + rel, sib, "core")

    early = lax.rem(L + swapped, 2)

    def start_y(b):
        mine = jnp.logical_and(straight, L == b)
        dl = lax.rem(L + b, 2)

        @pl.when(jnp.logical_not(mine))
        def _():
            arrive(statbuf.at[H, dl, 0], stat_r + 8 * H + 4 * dl)

        arrive(statbuf.at[1 - H, dl, 0], stat_r + 8 * (1 - H) + 4 * dl)
        for src in range(2):
            for dz in range(1, 4):
                arrive(statbuf.at[src, dl, dz], stat_r + 8 * src + 4 * dl + dz)
        summed = statbuf[0, dl, 0]
        for src, dz in [(0, 1), (0, 2), (0, 3), (1, 0), (1, 1), (1, 2), (1, 3)]:
            summed = summed + statbuf[src, dl, dz]
        column = jnp.transpose(jnp.concatenate([summed] * 16, axis=0))
        mean = column[:, 0:1] / width
        spread = column[:, 1:2] / width - mean * mean
        scale = lax.rsqrt(spread + EPS)
        gains = jnp.concatenate([statbuf[C, dl, 0, pl.ds(2 + k, 1)] for k in range(feat // rows)], axis=1)

        for n, part in enumerate(halves):

            @pl.when(jnp.logical_not(mine))
            def _():
                arrive(xraw.at[b, part], x_r + 2 * b + n)

            at = slice(n * half, (n + 1) * half)
            xbuf[C, 0, b, part] = ((xraw[b, part].astype(F32) - mean[at]) * scale[at] * gains).astype(BF16)
            copy(xbuf.at[C, 0, b, part], xbuf.at[C, 3, b, part], yp_r + 2 * b + n, up, "y")
            copy(xbuf.at[C, 0, b, part], xbuf.at[C, 1, b, part], ym_r + 2 * b + n, down, "y")
        to_sib(0, b)

    def relay_y(b):
        arrive(xbuf.at[C, 3, b, first], yp_r + 2 * b)
        copy(xbuf.at[C, 3, b, first], xbuf.at[C, 2, b, first], far_r, up, "y")
        arrive(xbuf.at[C, 1, b, first], ym_r + 2 * b)
        arrive(xbuf.at[C, 1, b, second], ym_r + 2 * b + 1)
        copy(xbuf.at[C, 1, b, second], xbuf.at[C, 2, b, second], far_r, down, "y")
        to_sib(1, b)
        arrive(xbuf.at[C, 3, b, second], yp_r + 2 * b + 1)
        to_sib(3, b)

    def far_y():
        arrive(xbuf.at[C, 2], far_r)
        for b in range(2):
            to_sib(2, b)

    start_y(early)
    start_y(1 - early)
    send_w1(0, near[1])
    for j in range(1, CHUNKS):
        for dev in near:
            send_w1(j, dev)
    for f in range(PARTS):
        for dev in near:
            send_w2(f, dev)

    n_items = 4 * CHUNKS
    r1_r, r2_r = sems("r", n_items), sems("r", n_items)
    near_r, far_h = sems("r", 8), sems("r", 4)
    e_r = sems("r", 4 * PARTS)
    zp, zm, z2 = lax.rem(Z + 1, 4), lax.rem(Z + 3, 4), lax.rem(Z + 2, 4)
    seen_w, seen_x = set(), set()

    def s1(j, rel):
        i = 4 * j + rel
        if j not in seen_w:
            seen_w.add(j)
            arrive(w1buf.at[j], w1_r + j)
        if rel not in seen_x:
            seen_x.add(rel)
            arrive(xbuf.at[1 - C, rel], sib_r + rel)

        @pl.loop(0, 2)
        def _(b):
            features = jnp.concatenate([xbuf[0, rel, b], xbuf[1, rel, b]], axis=1)
            weights = w1buf[j].reshape(2 * feat, WIDE)
            acc = jnp.dot(features, weights, preferred_element_type=F32)
            pbuf[i, b] = acc[:, :HEAD_DIM].astype(BF16)
            pbuf[i, 2 + b] = acc[:, HEAD_DIM:].astype(BF16)

        copy(pbuf.at[i, z2, pl.ds(0, half)], r1.at[0, i], r1_r + i, fwd, "r1")
        copy(pbuf.at[i, z2, pl.ds(half, half)], r1.at[1, i], r1_r + i, back, "r1")

    def s2(j, rel):
        i = 4 * j + rel
        arrive(r1.at[:, i], r1_r + i)
        pbuf[i, zp, pl.ds(0, half)] = (pbuf[i, zp, pl.ds(0, half)].astype(F32) + r1[0, i].astype(F32)).astype(BF16)
        copy(pbuf.at[i, zp], r2.at[0, i], r2_r + i, fwd, "r2")
        pbuf[i, zm, pl.ds(half, half)] = (
            pbuf[i, zm, pl.ds(half, half)].astype(F32) + r1[1, i].astype(F32)
        ).astype(BF16)
        copy(pbuf.at[i, zm], r2.at[1, i], r2_r + i, back, "r2")

    def s3(j, rel):
        i = 4 * j + rel
        arrive(r2.at[:, i], r2_r + i)
        whole = (pbuf[i, Z].astype(F32) + r2[0, i].astype(F32) + r2[1, i].astype(F32)).astype(BF16)
        if j < 3:
            qkv[rel, j] = whole
        if j == 2:
            query = (head_norm(qkv[rel, 0].astype(F32)) * (1.0 / HEAD_DIM) ** 0.5).astype(BF16)
            keys = head_norm(qkv[rel, 1].astype(F32)).astype(BF16)
            scores = lax.dot_general(query, keys, (((1,), (1,)), ((), ())), preferred_element_type=F32)
            weights = jnp.exp(scores)
            probs = (weights / jnp.sum(weights, axis=-1, keepdims=True)).astype(BF16)
            hbuf[rel, Z, 0] = jnp.dot(probs, whole, preferred_element_type=F32).astype(BF16)
        if j >= 3:
            hbuf[rel, Z, j - 2] = gelu(whole.astype(F32)).astype(BF16)
        if j in (3, 5):
            k = (j - 3) // 2
            mine = hbuf.at[rel, Z, pl.ds(2 * k, 2)]
            copy(mine, mine, near_r + 2 * rel + k, fwd, "near")
            copy(mine, mine, near_r + 2 * rel + k, back, "near")

    def relay(k, rel):
        arrive(hbuf.at[rel, pl.ds(0, 2), pl.ds(2 * k, 2)], near_r + 2 * rel + k)
        top = hbuf.at[rel, zm, pl.ds(2 * k, 2), pl.ds(0, half)]
        copy(top, top, far_h + rel, fwd, "far")
        low = hbuf.at[rel, zp, pl.ds(2 * k, 2), pl.ds(half, half)]
        copy(low, low, far_h + rel, back, "far")

    seen_w2, seen_h = set(), set()

    def e1(f, rel):
        if f not in seen_w2:
            seen_w2.add(f)
            arrive(w2buf.at[:, f], w2_r + f)
        if rel not in seen_h:
            seen_h.add(rel)
            arrive(hbuf.at[rel, z2], far_h + rel)

        @pl.loop(0, 2)
        def _(b):
            hidden = jnp.concatenate([hbuf[rel, 2 * h + b, k] for k in range(4) for h in range(2)], axis=1)
            both = jnp.concatenate([w2buf[0, f], w2buf[1, f]], axis=1)
            whole = jnp.dot(hidden, both, preferred_element_type=F32).astype(BF16)
            for side in range(2):
                oall[side, rel, f, b] = whole[:, side * WIDE : (side + 1) * WIDE]

        copy(oall.at[1 - C, rel, f], osib.at[rel, f], e_r + rel * PARTS + f, sib, "cores")

    ry_r = sems("r", 3 * PARTS)
    xr_r = sems("r", 2 * PARTS)
    xr_s = sems("s", 2 * PARTS)

    def final_copy(b, f):
        return pltpu.make_async_remote_copy(
            src_ref=xsend.at[f, b], dst_ref=xrecv.at[f, L], send_sem=send_sem.at[xr_s + 2 * f + b],
            recv_sem=recv_sem.at[xr_r + 2 * f + L], device_id={"H": C, "L": b, "C": H}, device_id_type=MESH,
        )

    def e2(f, rel):
        arrive(osib.at[rel, f], e_r + rel * PARTS + f)
        ry = ry_r + 3 * f
        for b in range(2):
            total = oall[C, rel, f, b].astype(F32) + osib[rel, f, b].astype(F32)
            if rel == 1 and b == 0:
                arrive(ry1.at[f, 0], ry)
                total = total + ry1[f, 0].astype(F32)
            if rel == 3 and b == 1:
                arrive(ry1.at[f, 1], ry + 1)
                total = total + ry1[f, 1].astype(F32)
            if rel == 0:
                if b == 0:
                    arrive(ry2.at[f], ry + 2)
                xsend[f, b] = (total + ry2[f, 0, b].astype(F32) + ry2[f, 1, b].astype(F32)).astype(BF16)
                mine = jnp.logical_and(C == H, L == b)

                @pl.when(mine)
                def _():
                    xrecv[f, b] = xsend[f, b]

                @pl.when(jnp.logical_not(mine))
                def _():
                    final_copy(b, f).start()
            else:
                oall[C, rel, f, b] = total.astype(BF16)
        if rel == 2:
            copy(oall.at[C, 2, f, 0], ry1.at[f, 0], ry, up, "ry1")
            copy(oall.at[C, 2, f, 1], ry1.at[f, 1], ry + 1, down, "ry1")
        if rel == 1:
            copy(oall.at[C, 1, f], ry2.at[f, 0], ry + 2, up, "ry2")
        if rel == 3:
            copy(oall.at[C, 3, f], ry2.at[f, 1], ry + 2, down, "ry2")

    stages = {
        "y1": lambda a, rel: relay_y(early),
        "y2": lambda a, rel: relay_y(1 - early),
        "y3": lambda a, rel: far_y(),
        "s1": s1, "s2": s2, "s3": s3, "s4": relay, "e1": e1, "e2": e2,
    }
    for stage, a, rel in ORDER:
        stages[stage](a, rel)

    for f in range(PARTS):
        for b in range(2):

            @pl.when(jnp.logical_not(jnp.logical_and(C == H, L == b)))
            def _():
                arrive(xrecv.at[f, b], xr_r + 2 * f + b)

        columns = pl.ds(f * WIDE, WIDE)
        out[:, columns] = (
            tok[:, columns].astype(F32) + xrecv[f, 0].astype(F32) + xrecv[f, 1].astype(F32)
        ).astype(BF16)

    for n, r in enumerate(readers):
        unless(straight, r == (0, 0, 0), lambda: stat_copy(n).wait_send())
    whole = {
        "w1": w1buf, "w2": w2buf, "y": xbuf.at[0, pl.ds(0, 3)], "core": xbuf.at[0], "r1": r1, "r2": r2,
        "near": hbuf.at[pl.ds(0, 2)], "far": hbuf.at[0], "cores": osib, "ry1": ry1, "ry2": ry2,
    }
    for kind, (sem, total) in pending.items():
        ref = whole[kind]
        assert size(ref) == total, kind
        pltpu.make_async_remote_copy(
            src_ref=ref, dst_ref=ref, send_sem=send_sem.at[sem], recv_sem=recv_sem.at[0],
            device_id=sib, device_id_type=MESH,
        ).wait_send()
    for b in range(2):

        @pl.when(jnp.logical_not(jnp.logical_and(C == H, L == b)))
        def _():
            for n in range(2):
                token_copy(b, n).wait_send()

        @pl.when(jnp.logical_not(jnp.logical_and(C == H, L == b)))
        def _():
            for f in range(PARTS):
                final_copy(b, f).wait_send()

    assert count["s"] <= N_SEND and count["r"] <= N_RECV, count


def local(tokens, norm_gain, w_qkv, w_up, w_attn_out, w_down):
    rows, feat = tokens.shape
    width = feat * lax.axis_size("H") * lax.axis_size("Z")
    n_items = 4 * CHUNKS
    half = rows // 2
    vmem = pltpu.VMEM
    out_part = (PARTS, 2, rows, WIDE)
    scratch = [
        vmem((8, rows), F32),
        vmem((2, 2, 4, 8, rows), F32),
        vmem((2, rows, feat), BF16),
        vmem((2, 4, 2, rows, feat), BF16),
        vmem((CHUNKS, 2, feat, WIDE), BF16),
        vmem((2, PARTS, w_attn_out.shape[0] + w_down.shape[0], WIDE), BF16),
        vmem((n_items, 4, rows, HEAD_DIM), BF16),
        vmem((2, n_items, half, HEAD_DIM), BF16),
        vmem((2, n_items, rows, HEAD_DIM), BF16),
        vmem((4, 3, rows, HEAD_DIM), BF16),
        vmem((4, 4, 4, rows, HEAD_DIM), BF16),
        vmem((2, 4, *out_part), BF16),
        vmem((4, *out_part), BF16),
        vmem((PARTS, 2, rows, WIDE), BF16),
        vmem((PARTS, 2, 2, rows, WIDE), BF16),
        vmem(out_part, BF16),
        vmem(out_part, BF16),
        pltpu.SemaphoreType.DMA((N_SEND,)),
        pltpu.SemaphoreType.DMA((N_RECV,)),
    ]
    in_vmem = pl.BlockSpec(memory_space=pltpu.VMEM)
    anywhere = pl.BlockSpec(memory_space=pl.ANY)
    return pl.pallas_call(
        functools.partial(kernel, width),
        out_shape=jax.ShapeDtypeStruct((rows, feat), BF16),
        in_specs=[in_vmem] * 2 + [anywhere] * 4,
        out_specs=in_vmem,
        scratch_shapes=scratch,
        compiler_params=pltpu.CompilerParams(
            collective_id=0, has_side_effects=True, vmem_limit_bytes=60 * 1024 * 1024
        ),
        name="layer",
    )(tokens, norm_gain, w_qkv.transpose(1, 0, 2), w_up, w_attn_out, w_down)


def solution(mesh):
    torus = Mesh(mesh.devices.reshape(2, 4, 2, 2, 4), ("L", "Y", "C", "H", "Z"))
    in_specs = (P(DP, MP), P(MP), P(MP, None, DP), P(MP, DP), P(DP, MP), P(DP, MP))
    return jax.shard_map(local, mesh=torus, in_specs=in_specs, out_specs=P(DP, MP), check_vma=False)
```
